256 devices in a mesh: gx: 8 (over z), gy: 32 (over y, x, core).
Axes of the slice: x: 4, y: 4, z: 8, core: 2. Of those that a mesh axis runs over, the one named last changes fastest.
Arguments:
- rhs: float32 [8, 32, 1, 3, 200, 128], P('gx', 'gy'), may hold values from -25 to 25
- stiff_inverse: bfloat16 [8, 32, 1, 1200, 1200], P('gx', 'gy'), may hold values from -2 to 6, as said below
- schur: bfloat16 [8, 32, 1, 1200, 1200], P('gx', 'gy'), may hold values from -2 to 6, as said below
- phi: bfloat16 [8, 32, 1, 24, 1200], P('gx', 'gy'), may hold values from -0.1875 to 0.1875
- coarse_inverse: float32 [1536, 1536], P(('gx', 'gy')), may hold values from -2 to 6, as said below
- incidence: int32 [8, 32, 1, 8], P('gx', 'gy'), may hold values from 0 to 511, as said below
- pairing: int32 [8, 32, 1, 3, 200], P('gx', 'gy'), may hold values from 0 to 199, as said below
Outputs:
- multipliers: float32 [8, 32, 1, 3, 200, 128], P('gx', 'gy')
- reduction: float32 [128], replicated
The draws below stay inside these ranges and needn't reach their ends.
Inputs may be any that keep to these rules, and one draw needn't show every extreme that they name: `stiff_inverse`: each block is symmetric positive definite. `schur`: each block is symmetric positive definite. `coarse_inverse`: symmetric positive definite. `incidence`: the corners of the subdomain grid, periodic in the first two dimensions, under an arbitrary numbering of the 512 nodes: corner c of subdomain (x, y, z) is the grid point (x + c % 2, y + (c // 2) % 2, z + c // 4), and subdomains that share a grid point name the same node. `pairing`: each row over the last dimension is a permutation of 0 to 199.
All inputs are finite; a program needn't handle non-finite values.
Results may differ from the reference program's by a relative error of at most 0.0027.
Values sent between devices are 32-bit elements; how exact they have to be, the bound alone decides.
No kernel may reach another device: no remote copies, remote signals or barrier semaphores. Data moves between devices by JAX's collectives and lax.ppermute only.
A program may use at most 64 MiB of HBM per device.

```python
import math
import jax
import jax.numpy as jnp
from jax import lax

ORDER = 1200
FACE = 200
CORNER = 24
LOADS = 128
SUB_DEV = 1
ITERS = 2
GRID_X = 8
GRID_Y = 32
NODES = 512
COARSE = 1536


def definite_block(key, size):
    noise = jax.random.normal(jax.random.fold_in(key, 1), (size, size), jnp.float32)
    coupled = (noise + noise.T) * (0.35 / math.sqrt(2.0 * size))
    diagonal = jax.random.uniform(jax.random.fold_in(key, 2), (size,), jnp.float32, 1.0, 2.0)
    block = coupled + jnp.diag(diagonal)
    return block


def block_stack(key):
    count = GRID_X * GRID_Y * SUB_DEV
    blocks = lax.map(lambda index: definite_block(jax.random.fold_in(key, index), ORDER).astype(jnp.bfloat16), jnp.arange(count))
    return blocks.reshape(GRID_X, GRID_Y, SUB_DEV, ORDER, ORDER)


def draw_stiff_inverse(key, part):
    return block_stack(jax.random.fold_in(key, 11))


def draw_schur(key, part):
    return block_stack(jax.random.fold_in(key, 23))


def draw_coarse_inverse(key, part):
    return definite_block(jax.random.fold_in(key, 37), COARSE)


def draw_rhs(key, part):
    count = GRID_X * GRID_Y * SUB_DEV
    shape = (GRID_X, GRID_Y, SUB_DEV, 3, FACE, LOADS)
    ramp = (jnp.arange(count, dtype=jnp.float32) / max(count - 1, 1)).reshape(GRID_X, GRID_Y, SUB_DEV, 1, 1, 1)
    scale = jnp.exp(math.log(3.0) * ramp)
    base = jax.random.truncated_normal(jax.random.fold_in(key, 63), -4.0, 4.0, shape, jnp.float32)
    return base * scale


def draw_incidence(key, part):
    dof_numbering = jax.random.permutation(jax.random.fold_in(key, 41), NODES).astype(jnp.int32)
    corner = jnp.arange(8, dtype=jnp.int32)
    first = jnp.arange(GRID_X, dtype=jnp.int32)[:, None, None, None] + corner % 2
    second = jnp.arange(GRID_Y, dtype=jnp.int32)[None, :, None, None] + corner // 2 % 2
    third = jnp.arange(SUB_DEV, dtype=jnp.int32)[None, None, :, None] + corner // 4
    node = (first % GRID_X * GRID_Y + second % GRID_Y) * (SUB_DEV + 1) + third
    return dof_numbering[node].astype(jnp.int32)


def draw_pairing(key, part):
    count = GRID_X * GRID_Y * SUB_DEV * 3
    subkeys = jax.random.split(jax.random.fold_in(key, 53), count)
    orderings = jax.vmap(lambda subkey: jax.random.permutation(subkey, FACE))(subkeys).astype(jnp.int32)
    return orderings.reshape(GRID_X, GRID_Y, SUB_DEV, 3, FACE)


def shard_levels(key, extent, pieces, low, high):
    def one(dim, blocks):
        draws = jax.random.uniform(jax.random.fold_in(jax.random.fold_in(key, 6), dim), (blocks,), jnp.float32, low / len(pieces), high / len(pieces))
        return jnp.repeat(jnp.exp(draws), extent[dim] // blocks).reshape((-1,) + (1,) * (len(extent) - dim - 1))

    loudness = one(*pieces[0])
    for cut in pieces[1:]:
        loudness = loudness * one(*cut)
    return loudness


def bell_draw(stream_key, dims, width, limit, pieces=(), held_as=jnp.bfloat16):
    values = jax.random.normal(stream_key, dims, jnp.float32) * width
    if len(pieces) > 0:
        values = shard_levels(stream_key, dims, pieces, -0.22, 0.18) * values
    return jnp.clip(values, min=-limit, max=limit).astype(held_as)


def setup_inputs(seed: int = 0) -> dict:
    key_list = jax.random.split(jax.random.key(seed), 8)
    rhs = draw_rhs(jax.random.fold_in(key_list[7], 71), 0)
    stiff_inverse = draw_stiff_inverse(jax.random.fold_in(key_list[7], 71), 0)
    schur = draw_schur(jax.random.fold_in(key_list[7], 71), 0)
    phi = bell_draw(key_list[3], (GRID_X, GRID_Y, SUB_DEV, CORNER, ORDER), ORDER ** -0.5, 0.1875, ((0, 8), (1, 32)))
    coarse_inverse = draw_coarse_inverse(jax.random.fold_in(key_list[7], 71), 0)
    incidence = draw_incidence(jax.random.fold_in(key_list[7], 71), 0)
    pairing = draw_pairing(jax.random.fold_in(key_list[7], 71), 0)
    return dict(rhs=rhs, stiff_inverse=stiff_inverse, schur=schur, phi=phi, coarse_inverse=coarse_inverse, incidence=incidence, pairing=pairing)


def reference(rhs, stiff_inverse, schur, phi, coarse_inverse, incidence, pairing):
    largest_index = lax.Precision.HIGHEST
    level = jnp.arange(SUB_DEV)[:, None]
    axis_id = jnp.arange(3)[None, :]
    active = jnp.where((level == SUB_DEV - 1) & (axis_id == 2), 0.0, 1.0)
    active = active.astype(jnp.float32)[None, None, :, :, None, None]
    inverse_pairing = jnp.argsort(pairing, axis=-1).astype(jnp.int32)
    coupling_matrix = phi.astype(jnp.float32)
    flat_ids = incidence.reshape(-1).astype(jnp.int32)

    def transpose_jump(values):
        masked = values * active
        moved = jnp.take_along_axis(masked, inverse_pairing[..., None], axis=4)
        lower_x = jnp.roll(moved[:, :, :, 0], 1, axis=0)
        lower_y = jnp.roll(moved[:, :, :, 1], 1, axis=1)
        lower_z = jnp.concatenate([jnp.zeros_like(moved[:, :, :1, 2]), moved[:, :, :-1, 2]], axis=2)
        return jnp.stack([-lower_x, masked[:, :, :, 0], -lower_y, masked[:, :, :, 1], -lower_z, masked[:, :, :, 2]], axis=3)

    def jump_field(field):
        upper_x = jnp.roll(field[:, :, :, 0], -1, axis=0)
        upper_y = jnp.roll(field[:, :, :, 2], -1, axis=1)
        upper_z = jnp.concatenate([field[:, :, 1:, 4], jnp.zeros_like(field[:, :, :1, 4])], axis=2)
        neighbour = jnp.stack([upper_x, upper_y, upper_z], axis=3)
        paired = jnp.take_along_axis(neighbour, pairing[..., None], axis=4)
        higher = jnp.stack([field[:, :, :, 1], field[:, :, :, 3], field[:, :, :, 5]], axis=3)
        return (higher - paired) * active

    def apply_local(matrices, field):
        flat_matrices = matrices.reshape(-1, ORDER, ORDER)
        flat_field = field.reshape(-1, ORDER, LOADS).astype(jnp.bfloat16)
        result = lax.map(lambda both: jnp.dot(both[0], both[1], preferred_element_type=jnp.float32), (flat_matrices, flat_field))
        return result.reshape(GRID_X, GRID_Y, SUB_DEV, 6, FACE, LOADS)

    def operator(values):
        field = transpose_jump(values)
        corner_load = jnp.einsum('xyzco,xyzor->xyzcr', coupling_matrix, field.reshape(GRID_X, GRID_Y, SUB_DEV, ORDER, LOADS), precision=largest_index)
        coarse_load = jax.ops.segment_sum(corner_load.reshape(-1, 3, LOADS), flat_ids, num_segments=NODES).reshape(COARSE, LOADS)
        coarse_solution = jnp.dot(coarse_inverse, coarse_load, precision=largest_index)
        corner_values = coarse_solution.reshape(NODES, 3, LOADS)[flat_ids].reshape(GRID_X, GRID_Y, SUB_DEV, CORNER, LOADS)
        spread_operator = jnp.einsum('xyzco,xyzcr->xyzor', coupling_matrix, corner_values, precision=largest_index)
        displacement = apply_local(stiff_inverse, field) + spread_operator.reshape(GRID_X, GRID_Y, SUB_DEV, 6, FACE, LOADS)
        return jump_field(displacement)

    def precondition(values):
        field = 0.5 * transpose_jump(values)
        return 0.5 * jump_field(apply_local(schur, field))

    def inner_product(left, right):
        return jnp.sum(left * right, axis=(0, 1, 2, 3, 4))

    residual = rhs * active
    multipliers = jnp.zeros_like(residual)
    preconditioned = precondition(residual)
    energy = inner_product(residual, preconditioned)
    start_energy = energy
    direction = preconditioned
    for iteration in range(ITERS):
        product_field = operator(direction)
        alpha = energy / inner_product(direction, product_field)
        multipliers = multipliers + alpha * direction
        residual = residual - alpha * product_field
        preconditioned = precondition(residual)
        energy_next = inner_product(residual, preconditioned)
        if iteration + 1 < ITERS:
            direction = preconditioned + (energy_next / energy) * direction
        energy = energy_next
    return multipliers, energy / start_energy
```

```python
import functools

import jax
import jax.numpy as jnp
import numpy as np
from jax import lax
from jax.experimental import pallas as pl
from jax.experimental.pallas import tpu as pltpu
from jax.sharding import Mesh
from jax.sharding import PartitionSpec as P

GY = ("gy_0", "gy_1", "gy_2")
GX_GY = ("gx", "gy_0", "gy_1", "gy_2")
EXACT = lax.Precision.HIGHEST
GX, GYN = 8, 32
CHUNK = 16
NODES = 2 * GX * GYN
E_LANE, ID_LANE = 120, 121
F32, BF16 = jnp.float32, jnp.bfloat16


def corner_lanes():
    lanes = np.full((GX, 128), -1, np.int32)
    shifts = [(0, 0), (1, 0), (-1, 0), (0, 1), (0, -1)]
    for x in range(GX):
        for t, (dx, dy) in enumerate(shifts):
            for c in range(8):
                for i in range(3):
                    node_x = (x + dx + c % 2) % GX
                    j = 1 + dy + (c // 2) % 2
                    lanes[x, t * 24 + 3 * c + i] = j * 64 + i * 16 + node_x * 2 + c // 4
        lanes[x, E_LANE] = 48
        lanes[x, ID_LANE] = 112 + 2 * x
        lanes[x, ID_LANE + 1] = 113 + 2 * x
    return lanes


def in_three(a):
    high = a.astype(BF16)
    rest = a - high.astype(F32)
    middle = rest.astype(BF16)
    low = (rest - middle.astype(F32)).astype(BF16)
    return jnp.concatenate([high, middle, low], axis=0)


def added_up(stacked):
    rows = stacked.shape[0] // 3
    return stacked[:rows] + (stacked[rows : 2 * rows] + stacked[2 * rows :])


def dot(a, b):
    return lax.dot_general(a, b, (((1,), (0,)), ((), ())), preferred_element_type=F32)


def dot_rows(a, b):
    return lax.dot_general(a, b, (((1,), (1,)), ((), ())), preferred_element_type=F32)


def moved_lanes(a, start, to):
    by = (to - start) % 128
    return a if by == 0 else pltpu.roll(a, by, 1)


def lane_group(shape):
    return lax.broadcasted_iota(jnp.int32, shape, 1) // 16


def spread_kernel(got_ref, lanes_ref, out_ref):
    total = jnp.zeros((3 * CHUNK, 256), F32)
    for x in range(GX):
        total += dot(in_three(got_ref[x, 0:CHUNK, :]), lanes_ref[x])
    out_ref[...] = jnp.broadcast_to(added_up(total)[None], out_ref.shape)


def assembled_loads(me, got_ref, loads_ref):
    group = lane_group((CHUNK, 128))
    tiles = [[None] * 4 for _ in range(3)]
    energy = jnp.zeros((CHUNK, 128), F32)

    def left(k):
        return got_ref[lax.rem(me + (k + 31) % GYN, GYN), :, 0:128]

    def right(k):
        return got_ref[lax.rem(me + (k + 31) % GYN, GYN), :, 128:256]

    for k in range(GYN):
        low = right(k - 1) + left(k + 1)
        high = left(k) + right(k - 2)
        load = low + pltpu.roll(high, 64, 1)
        energy += left(k)
        for i in range(3):
            piece = jnp.where(group == k % 8, moved_lanes(load, i * 16, (k % 8) * 16), 0.0)
            old = tiles[i][k // 8]
            tiles[i][k // 8] = piece if old is None else old + piece
    for i in range(3):
        for q in range(4):
            loads_ref[:, i * 512 + q * 128 : i * 512 + (q + 1) * 128] = tiles[i][q]
    return energy


def own_rows(loads_ref, high_ref, low_ref):
    total = jnp.zeros((CHUNK, 48), F32)
    for i in range(3):
        a = loads_ref[:, i * 512 : (i + 1) * 512]
        high = a.astype(BF16)
        low = (a - high.astype(F32)).astype(BF16)
        both = dot_rows(jnp.concatenate([high, low], axis=0), high_ref[i * 48 : (i + 1) * 48, :])
        total += both[:CHUNK] + both[CHUNK:] + dot_rows(high, low_ref[i * 48 : (i + 1) * 48, :])
    return total


def send_rows(rows, energy, sums_ref, out_ref, energy_ref):
    wide = jnp.concatenate([rows, jnp.zeros((CHUNK, 80), F32)], axis=1)
    out_ref[:, 0:CHUNK, :] = jnp.broadcast_to(wide[None], (GYN, CHUNK, 128))
    out_ref[:, CHUNK : CHUNK + 8, :] = jnp.broadcast_to(sums_ref[...][None], (GYN, 8, 128))
    energy_ref[...] = energy


def first_solve_kernel(
    me_ref, got_ref, rows_ref, sums_ref, out_ref, loads_ref, energy_ref, high_ref, low_ref, place_ref, held
):
    me = me_ref[0]
    energy = assembled_loads(me, got_ref, loads_ref)
    group = lane_group((8, 128))
    ids = []
    for q in range(4):
        tile = jnp.zeros((8, 128), F32)
        for n in range(8):
            left = got_ref[lax.rem(me + (q * 8 + n + 31) % GYN, GYN), 0:8, 0:128]
            tile += jnp.where(group == n, moved_lanes(left, 112, n * 16), 0.0)
        ids.append(tile[0:1])
    ids = jnp.concatenate(ids, axis=1).astype(jnp.int32)
    row = lax.broadcasted_iota(jnp.int32, (NODES, NODES), 0)
    by_id = jnp.where(row == ids, 1.0, 0.0).astype(BF16)
    place = (ids % 64 // 2) * 16 + (ids // 64) * 2 + ids % 2
    place_ref[...] = jnp.where(row == place, 1.0, 0.0).astype(BF16)
    for x in range(GX):
        for q in range(4):
            for column in range(3):
                for i in range(3):
                    start = CHUNK + q * 24 + column * 8 + i * 2
                    at = column * 48 + i * 16 + x * 2
                    held[at : at + 2, q * 128 : (q + 1) * 128] = rows_ref[x, start : start + 2, :]
    ordered = added_up(dot(in_three(held[...]), by_id))
    high = ordered.astype(BF16)
    high_ref[...] = high
    low_ref[...] = (ordered - high.astype(F32)).astype(BF16)
    rows = own_rows(loads_ref, high_ref, low_ref)
    send_rows(rows, energy, sums_ref, out_ref, energy_ref)


def next_solve_kernel(me_ref, got_ref, high_ref, low_ref, sums_ref, out_ref, loads_ref, energy_ref):
    energy = assembled_loads(me_ref[0], got_ref, loads_ref)
    rows = own_rows(loads_ref, high_ref, low_ref)
    send_rows(rows, energy, sums_ref, out_ref, energy_ref)


def lane_sum(a, b_ref, shape):
    total = jnp.zeros((CHUNK, 1), F32)
    for i in range(3):
        total += jnp.sum(a[:, i * 512 : (i + 1) * 512] * b_ref[i * CHUNK : (i + 1) * CHUNK, :], axis=1, keepdims=True)
    return jnp.broadcast_to(total, shape)


def pick_kernel(got_ref, loads_ref, energy_ref, place_ref, lanes_ref, before_ref, out_ref, grid_ref):
    group = lane_group((CHUNK, 128))
    tiles = [[None] * 4 for _ in range(3)]
    sums = jnp.zeros((8, 128), F32)
    for k in range(GYN):
        rows = got_ref[k, 0:CHUNK, :]
        sums += got_ref[k, CHUNK : CHUNK + 8, :]
        for i in range(3):
            piece = jnp.where(group == k % 8, moved_lanes(rows, i * 16, (k % 8) * 16), 0.0)
            old = tiles[i][k // 8]
            tiles[i][k // 8] = piece if old is None else old + piece
    solution = jnp.concatenate([jnp.concatenate(tiles[i], axis=1) for i in range(3)], axis=0)
    grid_ref[...] = added_up(dot(in_three(solution), place_ref[...]))
    loads = loads_ref[...]
    shape = (CHUNK, 128)
    product = lane_sum(loads, grid_ref, shape)
    mixed = lane_sum(loads, before_ref, shape)
    lane = lax.broadcasted_iota(jnp.int32, shape, 1)
    halves = []
    for half in range(2):
        tile = jnp.zeros(shape, F32)
        for n in range(2):
            for i in range(3):
                at = n * 64 + i * 16
                near = grid_ref[i * CHUNK : (i + 1) * CHUNK, 0:128]
                tile = jnp.where(group == at // 16, moved_lanes(near, (half * 2 + n) * 16, at), tile)
        if half == 0:
            tile = jnp.where(lane == 48, energy_ref[...], tile)
            tile = jnp.where(lane >= 112, jnp.where(lane % 2 == 0, product, mixed), tile)
        halves.append(tile)
    near = in_three(jnp.concatenate(halves, axis=1))
    for x in range(GX):
        out_ref[x, 0:CHUNK, :] = added_up(dot_rows(near, lanes_ref[x]))
        out_ref[x, CHUNK : CHUNK + 8, :] = sums


def call(kernel, outs, smem=0, scratch=(), flops=2_000_000):
    vmem = pl.BlockSpec(memory_space=pltpu.VMEM)

    def run(*operands):
        specs = [pl.BlockSpec(memory_space=pltpu.SMEM)] * smem + [vmem] * (len(operands) - smem)
        return pl.pallas_call(
            kernel,
            out_shape=[jax.ShapeDtypeStruct(s, d) for s, d in outs],
            in_specs=specs,
            out_specs=[vmem] * len(outs),
            scratch_shapes=list(scratch),
            cost_estimate=pl.CostEstimate(flops=flops, bytes_accessed=1_000_000, transcendentals=0),
        )(*operands)

    return run


SENT = [((GYN, CHUNK + 8, 128), F32), ((CHUNK, 3 * NODES), F32), ((CHUNK, 128), F32)]
spread = call(spread_kernel, [((GYN, CHUNK, 256), F32)])
first_solve = call(
    first_solve_kernel,
    SENT + [((144, NODES), BF16), ((144, NODES), BF16), ((NODES, NODES), BF16)],
    smem=1,
    scratch=[pltpu.VMEM((144, NODES), F32)],
)
next_solve = call(next_solve_kernel, SENT, smem=1)
pick = call(pick_kernel, [((GX, CHUNK + 8, 128), F32), ((3 * CHUNK, NODES), F32)])


def ring(axis, by):
    peers = lax.axis_size(axis)
    return [(i, (i + by) % peers) for i in range(peers)]


def passed_along(array, axis, by):
    return lax.ppermute(array, axis, ring(axis, by))


def exchanged(array, axis):
    return lax.all_to_all(array, axis, split_axis=0, concat_axis=0, tiled=True)


def of_everyone(array, axis):
    copies = jnp.broadcast_to(array, (lax.axis_size(axis), *array.shape))
    return jnp.sum(exchanged(copies, axis), axis=0)


def local(rhs, stiff_inverse, schur, phi, coarse_inverse, incidence, pairing):
    face = rhs.shape[4]
    cases = rhs.shape[5]
    interface = 6 * face
    stiffness = stiff_inverse[0, 0, 0]
    schur_block = schur[0, 0, 0]
    coupling = phi[0, 0, 0].astype(F32).reshape(24, 6, face)
    me = lax.axis_index(GY).astype(jnp.int32).reshape(1)
    active = jnp.array([1.0, 1.0, 0.0], F32)[:, None, None]
    within = jnp.array([1.0, 1.0, 1.0, 1.0, 0.0, 0.0], F32)[:, None, None]
    table = (pairing[0, 0, 0, :2, :, None] == jnp.arange(face)[None, None, :]).astype(F32)
    lanes = (jnp.asarray(corner_lanes())[:, :, None] == jnp.arange(256)[None, None, :]).astype(BF16)

    def moved(values):
        return jnp.einsum("akj,akr->ajr", table, values, precision=EXACT)

    def paired(values):
        return jnp.einsum("akj,ajr->akr", table, values, precision=EXACT)

    def exchange(field):
        up = moved(jnp.stack([field[1], field[3]]))
        below = (passed_along(up[0], "gx", 1), passed_along(up[1], GY, 1))
        above = (passed_along(field[0], "gx", -1), passed_along(field[2], GY, -1))
        return below, above

    def jumps(field, received):
        below, above = received
        above = paired(jnp.stack(above))
        other = jnp.stack([below[0], above[0], below[1], above[1], jnp.zeros_like(above[0]), jnp.zeros_like(above[0])])
        return (field - other) * within

    def times(matrix, field):
        low = field.reshape(interface, cases).astype(BF16)
        return jnp.dot(matrix, low, preferred_element_type=F32).reshape(6, face, cases)

    def inner(a, b):
        return jnp.sum(a * b, axis=(0, 1))

    residual = rhs[0, 0, 0] * active
    across = jnp.transpose(coupling, (1, 2, 0))
    both = jnp.concatenate(
        [residual[:2], jnp.stack([across[1], across[3]]), jnp.zeros((2, face, 104), F32)], axis=2
    )
    both = moved(both)
    below = (passed_along(both[0], "gx", 1), passed_along(both[1], GY, 1))
    above = (passed_along(across[0], "gx", -1), passed_along(across[2], GY, -1))
    none = jnp.zeros((face, cases), F32)
    start_field = jnp.stack(
        [-below[0][:, :cases], residual[0], -below[1][:, :cases], residual[1], none, residual[2]]
    )
    above = paired(jnp.stack(above))
    blank = jnp.zeros((6, face, 24), F32)
    neighbours = [
        blank.at[1].set(-above[0]),
        blank.at[0].set(-below[0][:, cases : cases + 24]),
        blank.at[3].set(-above[1]),
        blank.at[2].set(-below[1][:, cases : cases + 24]),
    ]
    reach = jnp.concatenate([across * within, *neighbours, jnp.zeros((6, face, 8), F32)], axis=2)
    reach = reach.reshape(interface, 128)

    mine = coarse_inverse.reshape(2, 3, 4, 128, 3)
    mine = jnp.transpose(mine, (2, 4, 1, 0, 3)).reshape(12, 6, 128)
    mine = jnp.concatenate([mine, jnp.zeros((12, 2, 128), F32)], axis=1).reshape(96, 128)
    ids = jnp.stack([incidence[0, 0, 0, 0], incidence[0, 0, 0, 4]]).astype(F32)

    def load_message(solved, energy):
        loads = 0.5 * lax.dot_general(
            solved.reshape(interface, cases), reach, (((0,), (0,)), ((), ())), precision=EXACT
        )
        lane = jnp.arange(128)[None, :]
        loads = jnp.where(lane == E_LANE, energy[:, None], loads)
        loads = jnp.where(lane == ID_LANE, ids[0], loads)
        loads = jnp.where(lane == ID_LANE + 1, ids[1], loads)
        return loads.reshape(GX, CHUNK, 128)

    def as_rows(*sums):
        return jnp.stack([*sums, *[jnp.zeros_like(sums[0])] * (8 - len(sums))])

    def returned(message):
        got = exchanged(message, "gx")
        corners = got[:, :CHUNK].reshape(cases, 128).T
        return corners, got[:, CHUNK:].sum(axis=0)

    def corner_field(corners):
        return jnp.dot(reach[:, :120], corners[:120], precision=EXACT).reshape(6, face, cases)

    half = 0.5 * start_field
    solved = times(schur_block, half)
    message = load_message(solved, jnp.sum(half * solved, axis=(0, 1)))
    message = jnp.concatenate([message, jnp.broadcast_to(mine, (GX, 96, 128))], axis=1)
    received = exchange(solved)
    got = exchanged(message, "gx")
    (sent,) = spread(got[:, :CHUNK], lanes)
    field = 0.5 * jumps(solved, received)
    stretched = times(stiffness, field)
    stretched_received = exchange(stretched)
    arrived = exchanged(sent, GY)
    sums = as_rows(inner(field, stretched))
    sent, loads, energy_lanes, high, low, place = first_solve(me, arrived, got, sums)
    energy_lanes = jnp.broadcast_to(energy_lanes[:, 48:49], (CHUNK, 128))
    arrived = exchanged(sent, GY)
    back, grid = pick(arrived, loads, energy_lanes, place, lanes, jnp.zeros((3 * CHUNK, NODES), F32))
    corners, sums = returned(back)
    start_energy = corners[E_LANE]
    curvature = sums[0] + corners[E_LANE + 1]
    alpha = start_energy / curvature
    multipliers = alpha * jnp.stack([field[1], field[3], field[5]])
    spread_field = jumps(stretched, stretched_received)
    half = half - (0.5 * alpha) * (spread_field + corner_field(corners))

    solved = times(schur_block, half)
    message = load_message(solved, jnp.sum(half * solved, axis=(0, 1)))
    received = exchange(solved)
    got = exchanged(message, "gx")
    (sent,) = spread(got, lanes)
    fresh = 0.5 * jumps(solved, received)
    fresh_stretched = times(stiffness, fresh)
    stretched_received = exchange(fresh_stretched)
    arrived = exchanged(sent, GY)
    sums = as_rows(inner(fresh, fresh_stretched), inner(fresh, stretched) + inner(field, fresh_stretched))
    sent, loads, energy_lanes = next_solve(me, arrived, high, low, sums)
    energy_lanes = jnp.broadcast_to(energy_lanes[:, 48:49], (CHUNK, 128))
    arrived = exchanged(sent, GY)
    back, _ = pick(arrived, loads, energy_lanes, place, lanes, grid)
    fresh_corners, sums = returned(back)
    energy = fresh_corners[E_LANE]
    ratio = energy / start_energy
    curvature = (
        sums[0] + fresh_corners[E_LANE + 1]
        + ratio * (sums[1] + 2.0 * fresh_corners[E_LANE + 2])
        + ratio * ratio * curvature
    )
    alpha = energy / curvature
    direction = fresh + ratio * field
    multipliers = multipliers + alpha * jnp.stack([direction[1], direction[3], direction[5]])
    spread_field = jumps(fresh_stretched, stretched_received) + ratio * spread_field
    half = half - (0.5 * alpha) * (spread_field + corner_field(fresh_corners + ratio * corners))
    energy = jnp.sum(half * times(schur_block, half), axis=(0, 1))
    energy = of_everyone(of_everyone(energy, "gx"), GY)
    return (multipliers[None, None, None], energy / start_energy)


def solution(mesh):
    finer = Mesh(mesh.devices.reshape(mesh.shape["gx"], 4, 4, 2), ("gx", "gy_0", "gy_1", "gy_2"))
    in_specs = (
        P("gx", GY, None, None, None, None),
        P("gx", GY, None, None, None),
        P("gx", GY, None, None, None),
        P("gx", GY, None, None, None),
        P(GX_GY, None),
        P("gx", GY, None, None),
        P("gx", GY, None, None, None),
    )
    out_specs = (P("gx", GY, None, None, None, None), P())
    return jax.shard_map(local, mesh=finer, in_specs=in_specs, out_specs=out_specs, check_vma=False)
```

```python
import functools

import jax
import jax.numpy as jnp
import numpy as np
from jax import lax
from jax.experimental import pallas as pl
from jax.experimental.pallas import tpu as pltpu
from jax.sharding import Mesh
from jax.sharding import PartitionSpec as P

GY = ("gy_0", "gy_1", "gy_2")
GX_GY = ("gx", "gy_0", "gy_1", "gy_2")
EXACT = lax.Precision.HIGHEST
GX, GYN = 8, 32
CHUNK = 16
NODES = 2 * GX * GYN
E_LANE, ID_LANE = 120, 121
F32, BF16 = jnp.float32, jnp.bfloat16


def corner_lanes():
    lanes = np.full((GX, 128), -1, np.int32)
    shifts = [(0, 0), (1, 0), (-1, 0), (0, 1), (0, -1)]
    for x in range(GX):
        for t, (dx, dy) in enumerate(shifts):
            for c in range(8):
                for i in range(3):
                    node_x = (x + dx + c % 2) % GX
                    j = 1 + dy + (c // 2) % 2
                    lanes[x, t * 24 + 3 * c + i] = j * 64 + i * 16 + node_x * 2 + c // 4
        lanes[x, E_LANE] = 48
        lanes[x, ID_LANE] = 112 + 2 * x
        lanes[x, ID_LANE + 1] = 113 + 2 * x
    return lanes


def in_three(a):
    high = a.astype(BF16)
    rest = a - high.astype(F32)
    middle = rest.astype(BF16)
    low = (rest - middle.astype(F32)).astype(BF16)
    return jnp.concatenate([high, middle, low], axis=0)


def added_up(stacked):
    rows = stacked.shape[0] // 3
    return stacked[:rows] + (stacked[rows : 2 * rows] + stacked[2 * rows :])


def dot(a, b):
    return lax.dot_general(a, b, (((1,), (0,)), ((), ())), preferred_element_type=F32)


def dot_rows(a, b):
    return lax.dot_general(a, b, (((1,), (1,)), ((), ())), preferred_element_type=F32)


def moved_lanes(a, start, to):
    by = (to - start) % 128
    return a if by == 0 else pltpu.roll(a, by, 1)


def lane_group(shape):
    return lax.broadcasted_iota(jnp.int32, shape, 1) // 16


def spread_kernel(got_ref, lanes_ref, out_ref):
    total = jnp.zeros((3 * CHUNK, 256), F32)
    for x in range(GX):
        total += dot(in_three(got_ref[x, 0:CHUNK, :]), lanes_ref[x])
    out_ref[...] = jnp.broadcast_to(added_up(total)[None], out_ref.shape)


def assembled_loads(me, got_ref, loads_ref):
    group = lane_group((CHUNK, 128))
    tiles = [[None] * 4 for _ in range(3)]
    energy = jnp.zeros((CHUNK, 128), F32)

    def left(k):
        return got_ref[lax.rem(me + (k + 31) % GYN, GYN), :, 0:128]

    def right(k):
        return got_ref[lax.rem(me + (k + 31) % GYN, GYN), :, 128:256]

    for k in range(GYN):
        low = right(k - 1) + left(k + 1)
        high = left(k) + right(k - 2)
        load = low + pltpu.roll(high, 64, 1)
        energy += left(k)
        for i in range(3):
            piece = jnp.where(group == k % 8, moved_lanes(load, i * 16, (k % 8) * 16), 0.0)
            old = tiles[i][k // 8]
            tiles[i][k // 8] = piece if old is None else old + piece
    for i in range(3):
        for q in range(4):
            loads_ref[:, i * 512 + q * 128 : i * 512 + (q + 1) * 128] = tiles[i][q]
    return energy


def own_rows(loads_ref, high_ref, low_ref):
    total = jnp.zeros((CHUNK, 48), F32)
    for i in range(3):
        a = loads_ref[:, i * 512 : (i + 1) * 512]
        high = a.astype(BF16)
        low = (a - high.astype(F32)).astype(BF16)
        both = dot_rows(jnp.concatenate([high, low], axis=0), high_ref[i * 48 : (i + 1) * 48, :])
        total += both[:CHUNK] + both[CHUNK:] + dot_rows(high, low_ref[i * 48 : (i + 1) * 48, :])
    return total


def send_rows(rows, energy, sums_ref, out_ref, energy_ref):
    wide = jnp.concatenate([rows, jnp.zeros((CHUNK, 80), F32)], axis=1)
    tile = wide[0:8] + pltpu.roll(wide[8:16], 48, 1)
    row = lax.broadcasted_iota(jnp.int32, (8, 128), 0)
    group = lane_group((8, 128))
    for n in range(2):
        spread_row = jnp.broadcast_to(sums_ref[n : n + 1, :], (8, 128))
        for r in range(8):
            here = (row == r) & (group == 6 + n)
            tile = jnp.where(here, moved_lanes(spread_row, r * 16, 96 + n * 16), tile)
    out_ref[...] = jnp.broadcast_to(tile[None], (GYN, 8, 128))
    energy_ref[...] = energy


def rows_of_sums(tile):
    row = lax.broadcasted_iota(jnp.int32, (8, 128), 0)
    group = lane_group((8, 128))
    out = jnp.zeros((8, 128), F32)
    for n in range(2):
        for r in range(8):
            whole = jnp.broadcast_to(tile[r : r + 1, :], (8, 128))
            out = jnp.where((row == n) & (group == r), moved_lanes(whole, 96 + n * 16, r * 16), out)
    return out


def first_solve_kernel(
    me_ref, got_ref, rows_ref, sums_ref, out_ref, loads_ref, energy_ref, high_ref, low_ref, place_ref, held
):
    me = me_ref[0]
    energy = assembled_loads(me, got_ref, loads_ref)
    group = lane_group((8, 128))
    ids = []
    for q in range(4):
        tile = jnp.zeros((8, 128), F32)
        for n in range(8):
            left = got_ref[lax.rem(me + (q * 8 + n + 31) % GYN, GYN), 0:8, 0:128]
            tile += jnp.where(group == n, moved_lanes(left, 112, n * 16), 0.0)
        ids.append(tile[0:1])
    ids = jnp.concatenate(ids, axis=1).astype(jnp.int32)
    row = lax.broadcasted_iota(jnp.int32, (NODES, NODES), 0)
    by_id = jnp.where(row == ids, 1.0, 0.0).astype(BF16)
    place = (ids % 64 // 2) * 16 + (ids // 64) * 2 + ids % 2
    place_ref[...] = jnp.where(row == place, 1.0, 0.0).astype(BF16)
    for x in range(GX):
        for q in range(4):
            for column in range(3):
                for i in range(3):
                    start = CHUNK + q * 24 + column * 8 + i * 2
                    at = column * 48 + i * 16 + x * 2
                    held[at : at + 2, q * 128 : (q + 1) * 128] = rows_ref[x, start : start + 2, :]
    ordered = added_up(dot(in_three(held[...]), by_id))
    high = ordered.astype(BF16)
    high_ref[...] = high
    low_ref[...] = (ordered - high.astype(F32)).astype(BF16)
    rows = own_rows(loads_ref, high_ref, low_ref)
    send_rows(rows, energy, sums_ref, out_ref, energy_ref)


def next_solve_kernel(me_ref, got_ref, high_ref, low_ref, sums_ref, out_ref, loads_ref, energy_ref):
    energy = assembled_loads(me_ref[0], got_ref, loads_ref)
    rows = own_rows(loads_ref, high_ref, low_ref)
    send_rows(rows, energy, sums_ref, out_ref, energy_ref)


def lane_sum(a, b_ref, shape):
    total = jnp.zeros((CHUNK, 1), F32)
    for i in range(3):
        total += jnp.sum(a[:, i * 512 : (i + 1) * 512] * b_ref[i * CHUNK : (i + 1) * CHUNK, :], axis=1, keepdims=True)
    return jnp.broadcast_to(total, shape)


def pick_kernel(got_ref, loads_ref, energy_ref, place_ref, lanes_ref, *rest):
    before_ref = rest[0] if len(rest) == 3 else None
    out_ref, grid_ref = rest[-2:]
    group = lane_group((CHUNK, 128))
    tiles = [[None] * 4 for _ in range(3)]
    sums = jnp.zeros((8, 128), F32)
    for k in range(GYN):
        rows = got_ref[k]
        sums += rows
        for i in range(3):
            to = (k % 8) * 16
            both = [moved_lanes(rows, i * 16, to), moved_lanes(rows, 48 + i * 16, to)]
            piece = jnp.where(group == k % 8, jnp.concatenate(both, axis=0), 0.0)
            old = tiles[i][k // 8]
            tiles[i][k // 8] = piece if old is None else old + piece
    solution = jnp.concatenate([jnp.concatenate(tiles[i], axis=1) for i in range(3)], axis=0)
    grid_ref[...] = added_up(dot(in_three(solution), place_ref[...]))
    loads = loads_ref[...]
    shape = (CHUNK, 128)
    product = lane_sum(loads, grid_ref, shape)
    mixed = product if before_ref is None else lane_sum(loads, before_ref, shape)
    lane = lax.broadcasted_iota(jnp.int32, shape, 1)
    halves = []
    for half in range(2):
        tile = jnp.zeros(shape, F32)
        for n in range(2):
            for i in range(3):
                at = n * 64 + i * 16
                near = grid_ref[i * CHUNK : (i + 1) * CHUNK, 0:128]
                tile = jnp.where(group == at // 16, moved_lanes(near, (half * 2 + n) * 16, at), tile)
        if half == 0:
            tile = jnp.where(lane == 48, energy_ref[...], tile)
            tile = jnp.where(lane >= 112, jnp.where(lane % 2 == 0, product, mixed), tile)
        halves.append(tile)
    near = in_three(jnp.concatenate(halves, axis=1))
    sums = rows_of_sums(sums)
    for x in range(GX):
        out_ref[x, 0:CHUNK, :] = added_up(dot_rows(near, lanes_ref[x]))
        out_ref[x, CHUNK : CHUNK + 8, :] = sums


def wide_three(a):
    high = a.astype(BF16)
    rest = a - high.astype(F32)
    middle = rest.astype(BF16)
    low = (rest - middle.astype(F32)).astype(BF16)
    return jnp.concatenate([high, middle, low], axis=1)


def wide_sum(a):
    width = a.shape[1] // 3
    return a[:, :width] + (a[:, width : 2 * width] + a[:, 2 * width :])


def dot_columns(a, b):
    return lax.dot_general(a, b, (((0,), (0,)), ((), ())), preferred_element_type=F32)


def faces_of(ref, n, face):
    return ref[n * face : (n + 1) * face, :]


def send_faces(values_ref, table_ref, outs, face):
    up_x, up_y, low_x, low_y = outs
    up_x[...] = wide_sum(dot(table_ref[0], wide_three(faces_of(values_ref, 1, face))))
    up_y[...] = wide_sum(dot(table_ref[1], wide_three(faces_of(values_ref, 3, face))))
    low_x[...] = faces_of(values_ref, 0, face)
    low_y[...] = faces_of(values_ref, 2, face)


def jump_faces(values_ref, received, table_ref, face):
    below_x, below_y, above_x, above_y = received
    up = [wide_sum(dot_columns(table_ref[a], wide_three(ref[...]))) for a, ref in ((0, above_x), (1, above_y))]
    own = [faces_of(values_ref, n, face) for n in range(6)]
    return [
        own[0] - below_x[...], own[1] - up[0], own[2] - below_y[...], own[3] - up[1], 0.0 * own[4], 0.0 * own[5]
    ]


def column_sum(a, b):
    return jnp.sum(a * b, axis=0, keepdims=True)


def write_rows(ref, rows):
    ref[...] = jnp.concatenate([*rows, jnp.zeros((8 - len(rows), rows[0].shape[1]), F32)], axis=0)


def loads_of(solved_ref, reach_ref, energy, ids, face):
    loads = jnp.zeros((128, 3 * 128), F32)
    for n in range(4):
        loads += dot(reach_ref[n], wide_three(faces_of(solved_ref, n, face)))
    loads = 0.5 * wide_sum(loads)
    row = lax.broadcasted_iota(jnp.int32, (128, 128), 0)
    loads = jnp.where(row == E_LANE, energy, loads)
    if ids is not None:
        number = jnp.where(row == ID_LANE, ids[0], jnp.where(row == ID_LANE + 1, ids[1], 0))
        loads = loads + number.astype(F32)
    return loads.T


def corner_faces(corners, reach_ref):
    pieces = wide_three(corners)
    return [wide_sum(dot_columns(reach_ref[n], pieces)) for n in range(4)]


def coupling_of(phi_ref, n, face):
    return phi_ref[...].astype(F32)[:, n * face : (n + 1) * face]


def start_kernel(rhs_ref, pairing_ref, phi_ref, plus_x, plus_y, minus_x, minus_y, table_ref):
    face = rhs_ref.shape[1]
    row = lax.broadcasted_iota(jnp.int32, (face, face), 0)
    for a, (plus, minus) in enumerate(((plus_x, minus_x), (plus_y, minus_y))):
        table = jnp.where(row == pairing_ref[a : a + 1, :], 1.0, 0.0).astype(BF16)
        table_ref[a] = table
        plus[0:face, :] = wide_sum(dot(table, wide_three(rhs_ref[a])))
        moved = dot_rows(coupling_of(phi_ref, 2 * a + 1, face).astype(BF16), table)
        moved = jnp.concatenate([moved, jnp.zeros((24, 256 - face), F32)], axis=1)
        plus[face : face + 24, :] = moved[:, :128]
        plus[face + 24 : face + 48, :] = moved[:, 128:]
        minus[...] = coupling_of(phi_ref, 2 * a, face)


def first_kernel(
    ids_ref, rhs_ref, below_x, below_y, above_x, above_y, phi_ref, table_ref, matrix_ref, rows_ref,
    half_ref, solved_ref, reach_ref, up_x, up_y, low_x, low_y, out_ref,
):
    face = rhs_ref.shape[1]
    none = jnp.zeros((face, 128), F32)
    half = [
        -0.5 * below_x[0:face, :], 0.5 * rhs_ref[0], -0.5 * below_y[0:face, :], 0.5 * rhs_ref[1], none, 0.0 * rhs_ref[2]
    ]
    for n in range(6):
        half_ref[n * face : (n + 1) * face, :] = half[n]
    solved_ref[...] = dot(matrix_ref[...], half_ref[...].astype(BF16))
    send_faces(solved_ref, table_ref, (up_x, up_y, low_x, low_y), face)

    def near(n, slot, other):
        parts = [coupling_of(phi_ref, n, face)] + [jnp.zeros((24, face), F32)] * 4 + [jnp.zeros((8, face), F32)]
        parts[slot] = -other
        reach_ref[n] = jnp.concatenate(parts, axis=0).astype(BF16)

    for a, (below, above) in enumerate(((below_x, above_x), (below_y, above_y))):
        near(2 * a + 1, 1 + 2 * a, dot(above[...].astype(BF16), table_ref[a]))
        under = jnp.concatenate([below[face : face + 24, :], below[face + 24 : face + 48, :]], axis=1)
        near(2 * a, 2 + 2 * a, under[:, :face])
    energy = column_sum(half_ref[...], solved_ref[...])
    loads = loads_of(solved_ref, reach_ref, energy, (ids_ref[0], ids_ref[4]), face)
    for x in range(GX):
        out_ref[x, 0:CHUNK, :] = loads[x * CHUNK : (x + 1) * CHUNK]
        out_ref[x, CHUNK : CHUNK + 96, :] = rows_ref[...]


def stretch_kernel(
    solved_ref, below_x, below_y, above_x, above_y, table_ref, matrix_ref, *rest
):
    face = below_x.shape[0]
    old = rest[:2] if len(rest) == 9 else None
    field_ref, stretched_ref, up_x, up_y, low_x, low_y, sums_ref = rest[-7:]
    jumped = jump_faces(solved_ref, (below_x, below_y, above_x, above_y), table_ref, face)
    for n in range(6):
        field_ref[n * face : (n + 1) * face, :] = 0.5 * jumped[n]
    stretched_ref[...] = dot(matrix_ref[...], field_ref[...].astype(BF16))
    send_faces(stretched_ref, table_ref, (up_x, up_y, low_x, low_y), face)
    rows = [column_sum(field_ref[...], stretched_ref[...])]
    if old is not None:
        old_field, old_stretched = old
        rows.append(
            column_sum(field_ref[...], old_stretched[...]) + column_sum(old_field[...], stretched_ref[...])
        )
    write_rows(sums_ref, rows)


def returned(got_ref):
    corners = jnp.concatenate([got_ref[x, 0:CHUNK, :] for x in range(GX)], axis=0).T
    sums = got_ref[0, CHUNK:, :]
    for x in range(1, GX):
        sums += got_ref[x, CHUNK:, :]
    return corners, sums


def turn_kernel(
    got_ref, half_ref, field_ref, stretched_ref, below_x, below_y, above_x, above_y, table_ref, reach_ref, matrix_ref,
    next_ref, solved_ref, image_ref, corners_ref, scalars_ref, up_x, up_y, low_x, low_y, out_ref,
):
    face = below_x.shape[0]
    corners, sums = returned(got_ref)
    corners_ref[...] = corners
    energy = corners[E_LANE : E_LANE + 1]
    curvature = sums[0:1] + corners[E_LANE + 1 : E_LANE + 2]
    alpha = energy / curvature
    write_rows(scalars_ref, [energy, curvature, alpha])
    jumped = jump_faces(stretched_ref, (below_x, below_y, above_x, above_y), table_ref, face)
    coarse = corner_faces(corners, reach_ref)
    for n in range(6):
        at = slice(n * face, (n + 1) * face)
        image = jumped[n] + coarse[n] if n < 4 else jumped[n]
        image_ref[at, :] = image
        next_ref[at, :] = half_ref[at, :] - (0.5 * alpha) * image
    solved_ref[...] = dot(matrix_ref[...], next_ref[...].astype(BF16))
    send_faces(solved_ref, table_ref, (up_x, up_y, low_x, low_y), face)
    energy = column_sum(next_ref[...], solved_ref[...])
    loads = loads_of(solved_ref, reach_ref, energy, None, face)
    for x in range(GX):
        out_ref[x] = loads[x * CHUNK : (x + 1) * CHUNK]


def last_kernel(
    got_ref, half_ref, field_ref, fresh_ref, stretched_ref, below_x, below_y, above_x, above_y, image_ref,
    corners_ref, scalars_ref, table_ref, reach_ref, matrix_ref, multipliers_ref, out_ref, held_ref,
):
    face = below_x.shape[0]
    corners, sums = returned(got_ref)
    start, curvature, alpha = scalars_ref[0:1], scalars_ref[1:2], scalars_ref[2:3]
    energy = corners[E_LANE : E_LANE + 1]
    ratio = energy / start
    mixed = sums[1:2] + 2.0 * corners[E_LANE + 2 : E_LANE + 3]
    curvature = sums[0:1] + corners[E_LANE + 1 : E_LANE + 2] + ratio * mixed + ratio * ratio * curvature
    step = energy / curvature
    jumped = jump_faces(stretched_ref, (below_x, below_y, above_x, above_y), table_ref, face)
    coarse = corner_faces(corners, reach_ref)
    for n in range(6):
        at = slice(n * face, (n + 1) * face)
        image = jumped[n] + coarse[n] if n < 4 else jumped[n]
        held_ref[at, :] = half_ref[at, :] - (0.5 * step) * (image + ratio * image_ref[at, :])
    for a in range(3):
        at = slice((2 * a + 1) * face, (2 * a + 2) * face)
        first = field_ref[at, :]
        multipliers_ref[a] = alpha * first + step * (fresh_ref[at, :] + ratio * first)
    solved = dot(matrix_ref[...], held_ref[...].astype(BF16))
    out_ref[...] = jnp.broadcast_to(column_sum(held_ref[...], solved)[None], out_ref.shape)


def pass_on_kernel(got_ref, out_ref):
    total = jnp.sum(got_ref[...], axis=0)
    out_ref[...] = jnp.broadcast_to(total[None], out_ref.shape)


def finish_kernel(got_ref, scalars_ref, out_ref):
    out_ref[...] = (jnp.sum(got_ref[...], axis=0) / jnp.broadcast_to(scalars_ref[0:1], (8, 128)))[0:1]


def call(kernel, outs, smem=0, scratch=(), flops=2_000_000):
    vmem = pl.BlockSpec(memory_space=pltpu.VMEM)

    def run(*operands, after=()):
        many = len(operands)

        def body(*refs):
            kernel(*refs[:many], *refs[many + len(after) :])

        specs = [pl.BlockSpec(memory_space=pltpu.SMEM)] * smem + [vmem] * (many - smem)
        return pl.pallas_call(
            body,
            name=kernel.__name__,
            out_shape=[jax.ShapeDtypeStruct(s, d) for s, d in outs],
            in_specs=specs + [pl.BlockSpec(memory_space=pl.ANY)] * len(after),
            out_specs=[vmem] * len(outs),
            scratch_shapes=list(scratch),
            cost_estimate=pl.CostEstimate(flops=flops, bytes_accessed=1_000_000, transcendentals=0),
        )(*operands, *after)

    return run


SENT = [((GYN, 8, 128), F32), ((CHUNK, 3 * NODES), F32), ((CHUNK, 128), F32)]
spread = call(spread_kernel, [((GYN, CHUNK, 256), F32)])
first_solve = call(
    first_solve_kernel,
    SENT + [((144, NODES), BF16), ((144, NODES), BF16), ((NODES, NODES), BF16)],
    smem=1,
    scratch=[pltpu.VMEM((144, NODES), F32)],
)
next_solve = call(next_solve_kernel, SENT, smem=1)
pick = call(pick_kernel, [((GX, CHUNK + 8, 128), F32), ((3 * CHUNK, NODES), F32)])


def passed_along(array, axis, by):
    peers = lax.axis_size(axis)
    return lax.ppermute(array, axis, [(i, (i + by) % peers) for i in range(peers)])


def passed_both_ways(up_x, up_y, low_x, low_y):
    return (
        passed_along(up_x, "gx", 1),
        passed_along(up_y, GY, 1),
        passed_along(low_x, "gx", -1),
        passed_along(low_y, GY, -1),
    )


def exchanged(array, axis):
    return lax.all_to_all(array, axis, split_axis=0, concat_axis=0, tiled=True)


def local(rhs, stiff_inverse, schur, phi, coarse_inverse, incidence, pairing):
    face = rhs.shape[4]
    interface = 6 * face
    rhs = rhs[0, 0, 0]
    stiffness = stiff_inverse[0, 0, 0]
    schur_block = schur[0, 0, 0]
    pairing = pairing[0, 0, 0]
    coupling = phi[0, 0, 0]
    me = lax.axis_index(GY).astype(jnp.int32).reshape(1)
    lanes = (jnp.asarray(corner_lanes())[:, :, None] == jnp.arange(256)[None, None, :]).astype(BF16)
    mine = coarse_inverse.reshape(2, 3, 4, 128, 3)
    mine = jnp.transpose(mine, (2, 4, 1, 0, 3)).reshape(12, 6, 128)
    mine = jnp.concatenate([mine, jnp.zeros((12, 2, 128), F32)], axis=1).reshape(96, 128)

    whole, faces = ((interface, 128), F32), [((face, 128), F32)] * 4
    big = 2 * interface * interface * 128
    *sent, table = call(
        start_kernel, [((face + 48, 128), F32)] * 2 + [((24, face), F32)] * 2 + [((2, face, face), BF16)]
    )(rhs, pairing, coupling)
    received = passed_both_ways(*sent)
    half, solved, reach, *sent, message = call(
        first_kernel,
        [whole, whole, ((4, 128, face), BF16), *faces, ((GX, CHUNK + 96, 128), F32)],
        smem=1,
        flops=big,
    )(incidence[0, 0, 0], rhs, *received, coupling, table, schur_block, mine)
    received = passed_both_ways(*sent)
    first_rows = exchanged(message, "gx")
    (sent,) = spread(first_rows, lanes, after=received)
    field, stretched, *faces_sent, sums = call(stretch_kernel, [whole, whole, *faces, ((8, 128), F32)], flops=big)(
        solved, *received, table, stiffness
    )
    received = passed_both_ways(*faces_sent)
    arrived = exchanged(sent, GY)
    sent, loads, energy, high, low, place = first_solve(me, arrived, first_rows, sums)
    back, grid = pick(exchanged(sent, GY), loads, energy, place, lanes, after=received)
    back = exchanged(back, "gx")
    half, solved, image, corners, scalars, *sent, message = call(
        turn_kernel,
        [whole, whole, whole, ((128, 128), F32), ((8, 128), F32), *faces, ((GX, CHUNK, 128), F32)],
        flops=big,
    )(back, half, field, stretched, *received, table, reach, schur_block)

    received = passed_both_ways(*sent)
    (sent,) = spread(exchanged(message, "gx"), lanes, after=received)
    fresh, fresh_stretched, *faces_sent, sums = call(
        stretch_kernel, [whole, whole, *faces, ((8, 128), F32)], flops=big
    )(solved, *received, table, stiffness, field, stretched)
    received = passed_both_ways(*faces_sent)
    sent, loads, energy = next_solve(me, exchanged(sent, GY), high, low, sums)
    back, _ = pick(exchanged(sent, GY), loads, energy, place, lanes, grid, after=received)
    back = exchanged(back, "gx")
    multipliers, energy = call(
        last_kernel,
        [((3, face, 128), F32), ((GX, 8, 128), F32)],
        scratch=[pltpu.VMEM((interface, 128), F32)],
        flops=big,
    )(
        back, half, field, fresh, fresh_stretched, *received, image, corners, scalars, table, reach, schur_block
    )
    (energy,) = call(pass_on_kernel, [((GYN, 8, 128), F32)])(exchanged(energy, "gx"))
    (reduction,) = call(finish_kernel, [((1, 128), F32)])(exchanged(energy, GY), scalars)
    return (multipliers[None, None, None], reduction[0])


def solution(mesh):
    finer = Mesh(mesh.devices.reshape(mesh.shape["gx"], 4, 4, 2), ("gx", "gy_0", "gy_1", "gy_2"))
    in_specs = (
        P("gx", GY, None, None, None, None),
        P("gx", GY, None, None, None),
        P("gx", GY, None, None, None),
        P("gx", GY, None, None, None),
        P(GX_GY, None),
        P("gx", GY, None, None),
        P("gx", GY, None, None, None),
    )
    out_specs = (P("gx", GY, None, None, None, None), P())
    return jax.shard_map(local, mesh=finer, in_specs=in_specs, out_specs=out_specs, check_vma=False)
```

```python
import functools

import jax
import jax.numpy as jnp
import numpy as np
from jax import lax
from jax.experimental import pallas as pl
from jax.experimental.pallas import tpu as pltpu
from jax.sharding import Mesh
from jax.sharding import PartitionSpec as P

GY = ("gy_0", "gy_1", "gy_2")
GX_GY = ("gx", "gy_0", "gy_1", "gy_2")
EXACT = lax.Precision.HIGHEST
GX, GYN = 8, 32
CHUNK = 16
NODES = 2 * GX * GYN
E_LANE, ID_LANE = 120, 121
F32, BF16 = jnp.float32, jnp.bfloat16


def corner_lanes():
    lanes = np.full(128, -1, np.int32)
    shifts = [(0, 0), (1, 0), (-1, 0), (0, 1), (0, -1)]
    for t, (dx, dy) in enumerate(shifts):
        for c in range(8):
            for i in range(3):
                j = 1 + dy + (c // 2) % 2
                lanes[t * 24 + 3 * c + i] = j * 64 + i * 16 + (dx + c % 2) % GX * 2 + c // 4
    lanes[E_LANE], lanes[ID_LANE], lanes[ID_LANE + 1] = 48, 112, 113
    return lanes


def halves_of(a, axis):
    high = a.astype(BF16)
    low = (a - high.astype(F32)).astype(BF16)
    return jnp.concatenate([high, low], axis=axis)


def in_two(a):
    return halves_of(a, 0)


def added_up(stacked):
    rows = stacked.shape[0] // 2
    return stacked[:rows] + stacked[rows:]


def dot(a, b):
    return lax.dot_general(a, b, (((1,), (0,)), ((), ())), preferred_element_type=F32)


def dot_rows(a, b):
    return lax.dot_general(a, b, (((1,), (1,)), ((), ())), preferred_element_type=F32)


def moved_lanes(a, start, to):
    by = (to - start) % 128
    return a if by == 0 else pltpu.roll(a, by, 1)


def lane_group(shape):
    return lax.broadcasted_iota(jnp.int32, shape, 1) // 16


def rolled_groups(a, by):
    by %= 16
    if by == 0:
        return a
    lane = lax.broadcasted_iota(jnp.int32, (a.shape[0], 128), 1) % 16
    tiles = [a[:, n : n + 128] for n in range(0, a.shape[1], 128)]
    return jnp.concatenate(
        [jnp.where(lane >= by, pltpu.roll(t, by, 1), pltpu.roll(t, 112 + by, 1)) for t in tiles], axis=1
    )


def spread_kernel(got_ref, lanes_ref, out_ref):
    loads = jnp.concatenate([got_ref[x, 0:CHUNK, :] for x in range(GX)], axis=0)
    placed = added_up(dot(in_two(loads), lanes_ref[...]))
    total = placed[0:CHUNK]
    for x in range(1, GX):
        total += rolled_groups(placed[x * CHUNK : (x + 1) * CHUNK], 2 * x)
    out_ref[...] = jnp.broadcast_to(total[None], out_ref.shape)


def assembled_loads(me, got_ref, loads_ref):
    group = lane_group((CHUNK, 128))
    tiles = [[None] * 4 for _ in range(3)]
    energy = jnp.zeros((CHUNK, 128), F32)

    def left(k):
        return got_ref[lax.rem(me + (k + 31) % GYN, GYN), :, 0:128]

    def right(k):
        return got_ref[lax.rem(me + (k + 31) % GYN, GYN), :, 128:256]

    for k in range(GYN):
        low = right(k - 1) + left(k + 1)
        high = left(k) + right(k - 2)
        load = low + pltpu.roll(high, 64, 1)
        energy += left(k)
        for i in range(3):
            piece = jnp.where(group == k % 8, moved_lanes(load, i * 16, (k % 8) * 16), 0.0)
            old = tiles[i][k // 8]
            tiles[i][k // 8] = piece if old is None else old + piece
    for i in range(3):
        for q in range(4):
            loads_ref[:, i * 512 + q * 128 : i * 512 + (q + 1) * 128] = tiles[i][q]
    energy = jnp.sum(jnp.where(group == 3, energy, 0.0), axis=1, keepdims=True)
    return jnp.broadcast_to(energy, (CHUNK, 128))


def own_rows(loads_ref, high_ref, low_ref):
    total = jnp.zeros((CHUNK, 48), F32)
    for i in range(3):
        a = loads_ref[:, i * 512 : (i + 1) * 512]
        high = a.astype(BF16)
        low = (a - high.astype(F32)).astype(BF16)
        both = dot_rows(jnp.concatenate([high, low], axis=0), high_ref[i * 48 : (i + 1) * 48, :])
        total += both[:CHUNK] + both[CHUNK:] + dot_rows(high, low_ref[i * 48 : (i + 1) * 48, :])
    return total


def send_rows(rows, energy, sums_ref, out_ref, energy_ref):
    wide = jnp.concatenate([rows, jnp.zeros((CHUNK, 80), F32)], axis=1)
    tile = wide[0:8] + pltpu.roll(wide[8:16], 48, 1)
    row = lax.broadcasted_iota(jnp.int32, (8, 128), 0)
    group = lane_group((8, 128))
    for n in range(2):
        spread_row = jnp.broadcast_to(sums_ref[n : n + 1, :], (8, 128))
        for r in range(8):
            here = (row == r) & (group == 6 + n)
            tile = jnp.where(here, moved_lanes(spread_row, r * 16, 96 + n * 16), tile)
    out_ref[...] = jnp.broadcast_to(tile[None], (GYN, 8, 128))
    energy_ref[...] = energy


def rows_of_sums(tile):
    row = lax.broadcasted_iota(jnp.int32, (8, 128), 0)
    group = lane_group((8, 128))
    out = jnp.zeros((8, 128), F32)
    for n in range(2):
        for r in range(8):
            whole = jnp.broadcast_to(tile[r : r + 1, :], (8, 128))
            out = jnp.where((row == n) & (group == r), moved_lanes(whole, 96 + n * 16, r * 16), out)
    return out


def first_solve_kernel(
    me_ref, got_ref, rows_ref, sums_ref, out_ref, loads_ref, energy_ref, high_ref, low_ref, place_ref, held
):
    me = me_ref[0]
    energy = assembled_loads(me, got_ref, loads_ref)
    group = lane_group((8, 128))
    ids = []
    for q in range(4):
        tile = jnp.zeros((8, 128), F32)
        for n in range(8):
            left = got_ref[lax.rem(me + (q * 8 + n + 31) % GYN, GYN), 0:8, 0:128]
            tile += jnp.where(group == n, moved_lanes(left, 112, n * 16), 0.0)
        ids.append(tile[0:1])
    ids = jnp.concatenate(ids, axis=1).astype(jnp.int32)
    row = lax.broadcasted_iota(jnp.int32, (NODES, NODES), 0)
    by_id = jnp.where(row == ids, 1.0, 0.0).astype(BF16)
    place = (ids % 64 // 2) * 16 + (ids // 64) * 2 + ids % 2
    place_ref[...] = jnp.where(row == place, 1.0, 0.0).astype(BF16)
    for x in range(GX):
        for q in range(4):
            for column in range(3):
                for i in range(3):
                    start = CHUNK + q * 18 + column * 6 + i * 2
                    at = column * 48 + i * 16 + x * 2
                    held[at : at + 2, q * 128 : (q + 1) * 128] = rows_ref[x, start : start + 2, :]
    ordered = added_up(dot(in_two(held[...]), by_id))
    high = ordered.astype(BF16)
    high_ref[...] = high
    low_ref[...] = (ordered - high.astype(F32)).astype(BF16)
    rows = own_rows(loads_ref, high_ref, low_ref)
    send_rows(rows, energy, sums_ref, out_ref, energy_ref)


def next_solve_kernel(me_ref, got_ref, high_ref, low_ref, sums_ref, out_ref, loads_ref, energy_ref):
    energy = assembled_loads(me_ref[0], got_ref, loads_ref)
    rows = own_rows(loads_ref, high_ref, low_ref)
    send_rows(rows, energy, sums_ref, out_ref, energy_ref)


def lane_sum(a, b_ref, shape):
    total = jnp.zeros((CHUNK, 1), F32)
    for i in range(3):
        total += jnp.sum(a[:, i * 512 : (i + 1) * 512] * b_ref[i * CHUNK : (i + 1) * CHUNK, :], axis=1, keepdims=True)
    return jnp.broadcast_to(total, shape)


def pick_kernel(got_ref, loads_ref, energy_ref, place_ref, lanes_ref, *rest):
    before_ref = rest[0] if len(rest) == 3 else None
    out_ref, grid_ref = rest[-2:]
    group = lane_group((CHUNK, 128))
    tiles = [[None] * 4 for _ in range(3)]
    sums = jnp.zeros((8, 128), F32)
    for k in range(GYN):
        rows = got_ref[k]
        sums += rows
        for i in range(3):
            to = (k % 8) * 16
            both = [moved_lanes(rows, i * 16, to), moved_lanes(rows, 48 + i * 16, to)]
            piece = jnp.where(group == k % 8, jnp.concatenate(both, axis=0), 0.0)
            old = tiles[i][k // 8]
            tiles[i][k // 8] = piece if old is None else old + piece
    solution = jnp.concatenate([jnp.concatenate(tiles[i], axis=1) for i in range(3)], axis=0)
    grid_ref[...] = added_up(dot(in_two(solution), place_ref[...]))
    loads = loads_ref[...]
    shape = (CHUNK, 128)
    product = lane_sum(loads, grid_ref, shape)
    mixed = product if before_ref is None else lane_sum(loads, before_ref, shape)
    lane = lax.broadcasted_iota(jnp.int32, shape, 1)
    halves = []
    for half in range(2):
        tile = jnp.zeros(shape, F32)
        for n in range(2):
            for i in range(3):
                at = n * 64 + i * 16
                near = grid_ref[i * CHUNK : (i + 1) * CHUNK, 0:128]
                tile = jnp.where(group == at // 16, moved_lanes(near, (half * 2 + n) * 16, at), tile)
        if half == 0:
            tile = jnp.where(group == 3, energy_ref[...], tile)
            tile = jnp.where(lane >= 112, jnp.where(lane % 2 == 0, product, mixed), tile)
        halves.append(tile)
    near = jnp.concatenate(halves, axis=1)
    near = jnp.concatenate([rolled_groups(near, -2 * x) for x in range(GX)], axis=0)
    picked = added_up(dot_rows(in_two(near), lanes_ref[...]))
    sums = rows_of_sums(sums)
    for x in range(GX):
        out_ref[x, 0:CHUNK, :] = picked[x * CHUNK : (x + 1) * CHUNK]
        out_ref[x, CHUNK : CHUNK + 8, :] = sums


def wide_two(a):
    return halves_of(a, 1)


def wide_sum(a):
    width = a.shape[1] // 2
    return a[:, :width] + a[:, width:]


def dot_columns(a, b):
    return lax.dot_general(a, b, (((0,), (0,)), ((), ())), preferred_element_type=F32)


def faces_of(ref, n, face):
    return ref[n * face : (n + 1) * face, :]


def send_faces(values_ref, table_ref, outs, face):
    up_x, up_y, low_x, low_y = outs
    up_x[...] = wide_sum(dot(table_ref[0], wide_two(faces_of(values_ref, 1, face))))
    up_y[...] = wide_sum(dot(table_ref[1], wide_two(faces_of(values_ref, 3, face))))
    low_x[...] = faces_of(values_ref, 0, face)
    low_y[...] = faces_of(values_ref, 2, face)


def jump_faces(values_ref, received, table_ref, face):
    below_x, below_y, above_x, above_y = received
    up = [wide_sum(dot_columns(table_ref[a], wide_two(ref[...]))) for a, ref in ((0, above_x), (1, above_y))]
    own = [faces_of(values_ref, n, face) for n in range(6)]
    return [
        own[0] - below_x[...], own[1] - up[0], own[2] - below_y[...], own[3] - up[1], 0.0 * own[4], 0.0 * own[5]
    ]


def column_sum(a, b):
    return jnp.sum(a * b, axis=0, keepdims=True)


def write_rows(ref, rows):
    ref[...] = jnp.concatenate([*rows, jnp.zeros((8 - len(rows), rows[0].shape[1]), F32)], axis=0)


def loads_of(solved_ref, reach_ref, energy, ids, face):
    loads = jnp.zeros((128, 2 * 128), F32)
    for n in range(4):
        loads += dot(reach_ref[n], wide_two(faces_of(solved_ref, n, face)))
    loads = 0.5 * wide_sum(loads)
    row = lax.broadcasted_iota(jnp.int32, (128, 128), 0)
    loads = jnp.where(row == E_LANE, energy, loads)
    if ids is not None:
        number = jnp.where(row == ID_LANE, ids[0], jnp.where(row == ID_LANE + 1, ids[1], 0))
        loads = loads + number.astype(F32)
    return loads.T


def corner_faces(corners, reach_ref):
    pieces = wide_two(corners)
    return [wide_sum(dot_columns(reach_ref[n], pieces)) for n in range(4)]


def coupling_of(phi_ref, n, face):
    return phi_ref[...].astype(F32)[:, n * face : (n + 1) * face]


def start_kernel(rhs_ref, pairing_ref, phi_ref, plus_x, plus_y, minus_x, minus_y, table_ref):
    face = rhs_ref.shape[1]
    row = lax.broadcasted_iota(jnp.int32, (face, face), 0)
    for a, (plus, minus) in enumerate(((plus_x, minus_x), (plus_y, minus_y))):
        table = jnp.where(row == pairing_ref[a : a + 1, :], 1.0, 0.0).astype(BF16)
        table_ref[a] = table
        plus[0:face, :] = wide_sum(dot(table, wide_two(rhs_ref[a])))
        moved = dot_rows(coupling_of(phi_ref, 2 * a + 1, face).astype(BF16), table)
        moved = jnp.concatenate([moved, jnp.zeros((24, 256 - face), F32)], axis=1)
        plus[face : face + 24, :] = moved[:, :128]
        plus[face + 24 : face + 48, :] = moved[:, 128:]
        minus[...] = coupling_of(phi_ref, 2 * a, face)


def first_kernel(
    ids_ref, rhs_ref, below_x, below_y, above_x, above_y, phi_ref, table_ref, matrix_ref, rows_ref,
    half_ref, solved_ref, reach_ref, up_x, up_y, low_x, low_y, out_ref,
):
    face = rhs_ref.shape[1]
    none = jnp.zeros((face, 128), F32)
    half = [
        -0.5 * below_x[0:face, :], 0.5 * rhs_ref[0], -0.5 * below_y[0:face, :], 0.5 * rhs_ref[1], none, 0.0 * rhs_ref[2]
    ]
    for n in range(6):
        half_ref[n * face : (n + 1) * face, :] = half[n]
    solved_ref[...] = dot(matrix_ref[...], half_ref[...].astype(BF16))
    send_faces(solved_ref, table_ref, (up_x, up_y, low_x, low_y), face)

    def near(n, slot, other):
        parts = [coupling_of(phi_ref, n, face)] + [jnp.zeros((24, face), F32)] * 4 + [jnp.zeros((8, face), F32)]
        parts[slot] = -other
        reach_ref[n] = jnp.concatenate(parts, axis=0).astype(BF16)

    for a, (below, above) in enumerate(((below_x, above_x), (below_y, above_y))):
        near(2 * a + 1, 1 + 2 * a, dot(above[...].astype(BF16), table_ref[a]))
        under = jnp.concatenate([below[face : face + 24, :], below[face + 24 : face + 48, :]], axis=1)
        near(2 * a, 2 + 2 * a, under[:, :face])
    energy = column_sum(half_ref[...], solved_ref[...])
    loads = loads_of(solved_ref, reach_ref, energy, (ids_ref[0], ids_ref[4]), face)
    for x in range(GX):
        out_ref[x, 0:CHUNK, :] = loads[x * CHUNK : (x + 1) * CHUNK]
        out_ref[x, CHUNK : CHUNK + 72, :] = rows_ref[...]


def stretch_kernel(
    solved_ref, below_x, below_y, above_x, above_y, table_ref, matrix_ref, *rest
):
    face = below_x.shape[0]
    old = rest[:2] if len(rest) == 10 else None
    field_ref, stretched_ref, upper_ref, up_x, up_y, low_x, low_y, sums_ref = rest[-8:]
    jumped = jump_faces(solved_ref, (below_x, below_y, above_x, above_y), table_ref, face)
    for n in range(6):
        field_ref[n * face : (n + 1) * face, :] = 0.5 * jumped[n]
        if n % 2 == 1:
            upper_ref[n // 2] = 0.5 * jumped[n]
    stretched_ref[...] = dot(matrix_ref[...], field_ref[...].astype(BF16))
    send_faces(stretched_ref, table_ref, (up_x, up_y, low_x, low_y), face)
    rows = [column_sum(field_ref[...], stretched_ref[...])]
    if old is not None:
        old_field, old_stretched = old
        rows.append(
            column_sum(field_ref[...], old_stretched[...]) + column_sum(old_field[...], stretched_ref[...])
        )
    write_rows(sums_ref, rows)


def returned(got_ref):
    corners = jnp.concatenate([got_ref[x, 0:CHUNK, :] for x in range(GX)], axis=0).T
    sums = got_ref[0, CHUNK:, :]
    for x in range(1, GX):
        sums += got_ref[x, CHUNK:, :]
    return corners, sums


def turn_kernel(
    got_ref, half_ref, stretched_ref, below_x, below_y, above_x, above_y, table_ref, reach_ref, matrix_ref,
    next_ref, solved_ref, image_ref, corners_ref, scalars_ref, up_x, up_y, low_x, low_y, out_ref,
):
    face = below_x.shape[0]
    corners, sums = returned(got_ref)
    corners_ref[...] = corners
    energy = corners[E_LANE : E_LANE + 1]
    curvature = sums[0:1] + corners[E_LANE + 1 : E_LANE + 2]
    alpha = energy / curvature
    write_rows(scalars_ref, [energy, curvature, alpha])
    jumped = jump_faces(stretched_ref, (below_x, below_y, above_x, above_y), table_ref, face)
    coarse = corner_faces(corners, reach_ref)
    for n in range(6):
        at = slice(n * face, (n + 1) * face)
        image = jumped[n] + coarse[n] if n < 4 else jumped[n]
        image_ref[at, :] = image
        next_ref[at, :] = half_ref[at, :] - (0.5 * alpha) * image
    solved_ref[...] = dot(matrix_ref[...], next_ref[...].astype(BF16))
    send_faces(solved_ref, table_ref, (up_x, up_y, low_x, low_y), face)
    energy = column_sum(next_ref[...], solved_ref[...])
    loads = loads_of(solved_ref, reach_ref, energy, None, face)
    for x in range(GX):
        out_ref[x] = loads[x * CHUNK : (x + 1) * CHUNK]


def last_kernel(
    got_ref, half_ref, upper_ref, fresh_ref, stretched_ref, below_x, below_y, above_x, above_y, image_ref,
    corners_ref, scalars_ref, table_ref, reach_ref, matrix_ref, multipliers_ref, out_ref, held_ref,
):
    face = below_x.shape[0]
    corners, sums = returned(got_ref)
    start, curvature, alpha = scalars_ref[0:1], scalars_ref[1:2], scalars_ref[2:3]
    energy = corners[E_LANE : E_LANE + 1]
    ratio = energy / start
    mixed = sums[1:2] + 2.0 * corners[E_LANE + 2 : E_LANE + 3]
    curvature = sums[0:1] + corners[E_LANE + 1 : E_LANE + 2] + ratio * mixed + ratio * ratio * curvature
    step = energy / curvature
    jumped = jump_faces(stretched_ref, (below_x, below_y, above_x, above_y), table_ref, face)
    coarse = corner_faces(corners, reach_ref)
    for n in range(6):
        at = slice(n * face, (n + 1) * face)
        image = jumped[n] + coarse[n] if n < 4 else jumped[n]
        held_ref[at, :] = half_ref[at, :] - (0.5 * step) * (image + ratio * image_ref[at, :])
    for a in range(3):
        first = upper_ref[a]
        multipliers_ref[a] = alpha * first + step * (fresh_ref[a] + ratio * first)
    solved = dot(matrix_ref[...], held_ref[...].astype(BF16))
    out_ref[...] = column_sum(held_ref[...], solved)


def call(kernel, outs, smem=0, scratch=(), flops=2_000_000):
    vmem = pl.BlockSpec(memory_space=pltpu.VMEM)

    def run(*operands, after=()):
        many = len(operands)

        def body(*refs):
            kernel(*refs[:many], *refs[many + len(after) :])

        specs = [pl.BlockSpec(memory_space=pltpu.SMEM)] * smem + [vmem] * (many - smem)
        return pl.pallas_call(
            body,
            name=kernel.__name__,
            out_shape=[jax.ShapeDtypeStruct(s, d) for s, d in outs],
            in_specs=specs + [pl.BlockSpec(memory_space=pl.ANY)] * len(after),
            out_specs=[vmem] * len(outs),
            scratch_shapes=list(scratch),
            cost_estimate=pl.CostEstimate(flops=flops, bytes_accessed=1_000_000, transcendentals=0),
        )(*operands, *after)

    return run


SENT = [((GYN, 8, 128), F32), ((CHUNK, 3 * NODES), F32), ((CHUNK, 128), F32)]
spread = call(spread_kernel, [((GYN, CHUNK, 256), F32)])
first_solve = call(
    first_solve_kernel,
    SENT + [((144, NODES), BF16), ((144, NODES), BF16), ((NODES, NODES), BF16)],
    smem=1,
    scratch=[pltpu.VMEM((144, NODES), F32)],
)
next_solve = call(next_solve_kernel, SENT, smem=1)
pick = call(pick_kernel, [((GX, CHUNK + 8, 128), F32), ((3 * CHUNK, NODES), F32)])


def passed_along(array, axis, by):
    peers = lax.axis_size(axis)
    return lax.ppermute(array, axis, [(i, (i + by) % peers) for i in range(peers)])


def passed_both_ways(up_x, up_y, low_x, low_y):
    return (
        passed_along(up_x, "gx", 1),
        passed_along(up_y, GY, 1),
        passed_along(low_x, "gx", -1),
        passed_along(low_y, GY, -1),
    )


def exchanged(array, axis):
    return lax.all_to_all(array, axis, split_axis=0, concat_axis=0, tiled=True)


def local(rhs, stiff_inverse, schur, phi, coarse_inverse, incidence, pairing):
    face = rhs.shape[4]
    interface = 6 * face
    rhs = rhs[0, 0, 0]
    stiffness = stiff_inverse[0, 0, 0]
    schur_block = schur[0, 0, 0]
    pairing = pairing[0, 0, 0]
    coupling = phi[0, 0, 0]
    me = lax.axis_index(GY).astype(jnp.int32).reshape(1)
    lanes = (jnp.asarray(corner_lanes())[:, None] == jnp.arange(256)[None, :]).astype(BF16)
    mine = coarse_inverse.reshape(2, 3, 4, 128, 3)
    mine = jnp.transpose(mine, (2, 4, 1, 0, 3)).reshape(72, 128)

    whole, upper, faces = ((interface, 128), F32), ((3, face, 128), F32), [((face, 128), F32)] * 4
    big = 2 * interface * interface * 128
    *sent, table = call(
        start_kernel, [((face + 48, 128), F32)] * 2 + [((24, face), F32)] * 2 + [((2, face, face), BF16)]
    )(rhs, pairing, coupling)
    received = passed_both_ways(*sent)
    half, solved, reach, *sent, message = call(
        first_kernel,
        [whole, whole, ((4, 128, face), BF16), *faces, ((GX, CHUNK + 72, 128), F32)],
        smem=1,
        flops=big,
    )(incidence[0, 0, 0], rhs, *received, coupling, table, schur_block, mine)
    received = passed_both_ways(*sent)
    first_rows = exchanged(message, "gx")
    (sent,) = spread(first_rows, lanes, after=received)
    field, stretched, direction, *faces_sent, sums = call(stretch_kernel, [whole, whole, upper, *faces, ((8, 128), F32)], flops=big)(
        solved, *received, table, stiffness
    )
    received = passed_both_ways(*faces_sent)
    arrived = exchanged(sent, GY)
    sent, loads, energy, high, low, place = first_solve(me, arrived, first_rows, sums)
    back, grid = pick(exchanged(sent, GY), loads, energy, place, lanes, after=received)
    back = exchanged(back, "gx")
    half, solved, image, corners, scalars, *sent, message = call(
        turn_kernel,
        [whole, whole, whole, ((128, 128), F32), ((8, 128), F32), *faces, ((GX, CHUNK, 128), F32)],
        flops=big,
    )(back, half, stretched, *received, table, reach, schur_block)

    received = passed_both_ways(*sent)
    (sent,) = spread(exchanged(message, "gx"), lanes, after=received)
    _, fresh_stretched, fresh, *faces_sent, sums = call(
        stretch_kernel, [whole, whole, upper, *faces, ((8, 128), F32)], flops=big
    )(solved, *received, table, stiffness, field, stretched)
    received = passed_both_ways(*faces_sent)
    sent, loads, energy = next_solve(me, exchanged(sent, GY), high, low, sums)
    back, _ = pick(exchanged(sent, GY), loads, energy, place, lanes, grid, after=received)
    back = exchanged(back, "gx")
    multipliers, energy = call(
        last_kernel,
        [((3, face, 128), F32), ((1, 128), F32)],
        scratch=[pltpu.VMEM((interface, 128), F32)],
        flops=big,
    )(
        back, half, direction, fresh, fresh_stretched, *received, image, corners, scalars, table, reach, schur_block
    )
    energy = jnp.sum(exchanged(jnp.broadcast_to(energy, (GX * GYN, 1, 128)), GX_GY), axis=(0, 1))
    return (multipliers[None, None, None], energy / scalars[0])


def solution(mesh):
    finer = Mesh(mesh.devices.reshape(mesh.shape["gx"], 4, 4, 2), ("gx", "gy_0", "gy_1", "gy_2"))
    in_specs = (
        P("gx", GY, None, None, None, None),
        P("gx", GY, None, None, None),
        P("gx", GY, None, None, None),
        P("gx", GY, None, None, None),
        P(GX_GY, None),
        P("gx", GY, None, None),
        P("gx", GY, None, None, None),
    )
    out_specs = (P("gx", GY, None, None, None, None), P())
    return jax.shard_map(local, mesh=finer, in_specs=in_specs, out_specs=out_specs, check_vma=False)
```

```python
import functools

import jax
import jax.numpy as jnp
import numpy as np
from jax import lax
from jax.experimental import pallas as pl
from jax.experimental.pallas import tpu as pltpu
from jax.sharding import Mesh
from jax.sharding import PartitionSpec as P

GY = ("gy_0", "gy_1", "gy_2")
GX_GY = ("gx", "gy_0", "gy_1", "gy_2")
EXACT = lax.Precision.HIGHEST
GX, GYN = 8, 32
CHUNK = 16
NODES = 2 * GX * GYN
VMEM_LIMIT = 55_000_000
E_LANE, ID_LANE = 120, 121
F32, BF16 = jnp.float32, jnp.bfloat16


def corner_lanes():
    lanes = np.full(128, -1, np.int32)
    shifts = [(0, 0), (1, 0), (-1, 0), (0, 1), (0, -1)]
    for t, (dx, dy) in enumerate(shifts):
        for c in range(8):
            for i in range(3):
                j = 1 + dy + (c // 2) % 2
                lanes[t * 24 + 3 * c + i] = j * 64 + i * 16 + (dx + c % 2) % GX * 2 + c // 4
    lanes[E_LANE], lanes[ID_LANE], lanes[ID_LANE + 1] = 48, 112, 113
    return lanes


def halves_of(a, axis):
    high = a.astype(BF16)
    low = (a - high.astype(F32)).astype(BF16)
    return jnp.concatenate([high, low], axis=axis)


def in_two(a):
    return halves_of(a, 0)


def added_up(stacked):
    rows = stacked.shape[0] // 2
    return stacked[:rows] + stacked[rows:]


def dot(a, b):
    return lax.dot_general(a, b, (((1,), (0,)), ((), ())), preferred_element_type=F32)


def dot_rows(a, b):
    return lax.dot_general(a, b, (((1,), (1,)), ((), ())), preferred_element_type=F32)


def moved_lanes(a, start, to):
    by = (to - start) % 128
    return a if by == 0 else pltpu.roll(a, by, 1)


def lane_group(shape):
    return lax.broadcasted_iota(jnp.int32, shape, 1) // 16


def rolled_groups(a, by):
    by %= 16
    if by == 0:
        return a
    lane = lax.broadcasted_iota(jnp.int32, (a.shape[0], 128), 1) % 16
    tiles = [a[:, n : n + 128] for n in range(0, a.shape[1], 128)]
    return jnp.concatenate(
        [jnp.where(lane >= by, pltpu.roll(t, by, 1), pltpu.roll(t, 112 + by, 1)) for t in tiles], axis=1
    )


def spread_kernel(got_ref, lanes_ref, out_ref):
    loads = jnp.concatenate([got_ref[x, 0:CHUNK, :] for x in range(GX)], axis=0)
    placed = added_up(dot(in_two(loads), lanes_ref[...]))
    total = placed[0:CHUNK]
    for x in range(1, GX):
        total += rolled_groups(placed[x * CHUNK : (x + 1) * CHUNK], 2 * x)
    out_ref[...] = jnp.broadcast_to(total[None], out_ref.shape)


def assembled_loads(me, got_ref, loads_ref):
    group = lane_group((CHUNK, 128))
    tiles = [[None] * 4 for _ in range(3)]
    energy = jnp.zeros((CHUNK, 128), F32)

    def left(k):
        return got_ref[lax.rem(me + (k + 31) % GYN, GYN), :, 0:128]

    def right(k):
        return got_ref[lax.rem(me + (k + 31) % GYN, GYN), :, 128:256]

    for k in range(GYN):
        low = right(k - 1) + left(k + 1)
        high = left(k) + right(k - 2)
        load = low + pltpu.roll(high, 64, 1)
        energy += left(k)
        for i in range(3):
            piece = jnp.where(group == k % 8, moved_lanes(load, i * 16, (k % 8) * 16), 0.0)
            old = tiles[i][k // 8]
            tiles[i][k // 8] = piece if old is None else old + piece
    for i in range(3):
        for q in range(4):
            loads_ref[:, i * 512 + q * 128 : i * 512 + (q + 1) * 128] = tiles[i][q]
    energy = jnp.sum(jnp.where(group == 3, energy, 0.0), axis=1, keepdims=True)
    return jnp.broadcast_to(energy, (CHUNK, 128))


def own_rows(loads_ref, high_ref, low_ref):
    total = jnp.zeros((CHUNK, 48), F32)
    for i in range(3):
        a = loads_ref[:, i * 512 : (i + 1) * 512]
        high = a.astype(BF16)
        low = (a - high.astype(F32)).astype(BF16)
        both = dot_rows(jnp.concatenate([high, low], axis=0), high_ref[i * 48 : (i + 1) * 48, :])
        total += both[:CHUNK] + both[CHUNK:] + dot_rows(high, low_ref[i * 48 : (i + 1) * 48, :])
    return total


def send_rows(rows, energy, sums_ref, out_ref, energy_ref):
    wide = jnp.concatenate([rows, jnp.zeros((CHUNK, 80), F32)], axis=1)
    tile = wide[0:8] + pltpu.roll(wide[8:16], 48, 1)
    row = lax.broadcasted_iota(jnp.int32, (8, 128), 0)
    group = lane_group((8, 128))
    for n in range(2):
        spread_row = jnp.broadcast_to(sums_ref[n : n + 1, :], (8, 128))
        for r in range(8):
            here = (row == r) & (group == 6 + n)
            tile = jnp.where(here, moved_lanes(spread_row, r * 16, 96 + n * 16), tile)
    out_ref[...] = jnp.broadcast_to(tile[None], (GYN, 8, 128))
    energy_ref[...] = energy


def rows_of_sums(tile):
    row = lax.broadcasted_iota(jnp.int32, (8, 128), 0)
    group = lane_group((8, 128))
    out = jnp.zeros((8, 128), F32)
    for n in range(2):
        for r in range(8):
            whole = jnp.broadcast_to(tile[r : r + 1, :], (8, 128))
            out = jnp.where((row == n) & (group == r), moved_lanes(whole, 96 + n * 16, r * 16), out)
    return out


def first_solve_kernel(
    me_ref, got_ref, rows_ref, sums_ref, out_ref, loads_ref, energy_ref, high_ref, low_ref, place_ref, held
):
    me = me_ref[0]
    energy = assembled_loads(me, got_ref, loads_ref)
    group = lane_group((8, 128))
    ids = []
    for q in range(4):
        tile = jnp.zeros((8, 128), F32)
        for n in range(8):
            left = got_ref[lax.rem(me + (q * 8 + n + 31) % GYN, GYN), 0:8, 0:128]
            tile += jnp.where(group == n, moved_lanes(left, 112, n * 16), 0.0)
        ids.append(tile[0:1])
    ids = jnp.concatenate(ids, axis=1).astype(jnp.int32)
    row = lax.broadcasted_iota(jnp.int32, (NODES, NODES), 0)
    by_id = jnp.where(row == ids, 1.0, 0.0).astype(BF16)
    place = (ids % 64 // 2) * 16 + (ids // 64) * 2 + ids % 2
    place_ref[...] = jnp.where(row == place, 1.0, 0.0).astype(BF16)
    for x in range(GX):
        for q in range(4):
            for column in range(3):
                for i in range(3):
                    start = CHUNK + q * 18 + column * 6 + i * 2
                    at = column * 48 + i * 16 + x * 2
                    held[at : at + 2, q * 128 : (q + 1) * 128] = rows_ref[x, start : start + 2, :]
    ordered = added_up(dot(in_two(held[...]), by_id))
    high = ordered.astype(BF16)
    high_ref[...] = high
    low_ref[...] = (ordered - high.astype(F32)).astype(BF16)
    rows = own_rows(loads_ref, high_ref, low_ref)
    send_rows(rows, energy, sums_ref, out_ref, energy_ref)


def next_solve_kernel(me_ref, got_ref, high_ref, low_ref, sums_ref, out_ref, loads_ref, energy_ref):
    energy = assembled_loads(me_ref[0], got_ref, loads_ref)
    rows = own_rows(loads_ref, high_ref, low_ref)
    send_rows(rows, energy, sums_ref, out_ref, energy_ref)


def lane_sum(a, b_ref, shape):
    total = jnp.zeros((CHUNK, 1), F32)
    for i in range(3):
        total += jnp.sum(a[:, i * 512 : (i + 1) * 512] * b_ref[i * CHUNK : (i + 1) * CHUNK, :], axis=1, keepdims=True)
    return jnp.broadcast_to(total, shape)


def pick_kernel(got_ref, loads_ref, energy_ref, place_ref, lanes_ref, *rest):
    before_ref = rest[0] if len(rest) == 3 else None
    out_ref, grid_ref = rest[-2:]
    group = lane_group((CHUNK, 128))
    tiles = [[None] * 4 for _ in range(3)]
    sums = jnp.zeros((8, 128), F32)
    for k in range(GYN):
        rows = got_ref[k]
        sums += rows
        for i in range(3):
            to = (k % 8) * 16
            both = [moved_lanes(rows, i * 16, to), moved_lanes(rows, 48 + i * 16, to)]
            piece = jnp.where(group == k % 8, jnp.concatenate(both, axis=0), 0.0)
            old = tiles[i][k // 8]
            tiles[i][k // 8] = piece if old is None else old + piece
    solution = jnp.concatenate([jnp.concatenate(tiles[i], axis=1) for i in range(3)], axis=0)
    grid_ref[...] = added_up(dot(in_two(solution), place_ref[...]))
    loads = loads_ref[...]
    shape = (CHUNK, 128)
    product = lane_sum(loads, grid_ref, shape)
    mixed = product if before_ref is None else lane_sum(loads, before_ref, shape)
    lane = lax.broadcasted_iota(jnp.int32, shape, 1)
    halves = []
    for half in range(2):
        tile = jnp.zeros(shape, F32)
        for n in range(2):
            for i in range(3):
                at = n * 64 + i * 16
                near = grid_ref[i * CHUNK : (i + 1) * CHUNK, 0:128]
                tile = jnp.where(group == at // 16, moved_lanes(near, (half * 2 + n) * 16, at), tile)
        if half == 0:
            tile = jnp.where(group == 3, energy_ref[...], tile)
            tile = jnp.where(lane >= 112, jnp.where(lane % 2 == 0, product, mixed), tile)
        halves.append(tile)
    near = jnp.concatenate(halves, axis=1)
    near = jnp.concatenate([rolled_groups(near, -2 * x) for x in range(GX)], axis=0)
    picked = added_up(dot_rows(in_two(near), lanes_ref[...]))
    sums = rows_of_sums(sums)
    for x in range(GX):
        out_ref[x, 0:CHUNK, :] = picked[x * CHUNK : (x + 1) * CHUNK]
        out_ref[x, CHUNK : CHUNK + 8, :] = sums


def wide_two(a):
    return halves_of(a, 1)


def wide_sum(a):
    width = a.shape[1] // 2
    return a[:, :width] + a[:, width:]


def dot_columns(a, b):
    return lax.dot_general(a, b, (((0,), (0,)), ((), ())), preferred_element_type=F32)


def faces_of(ref, n, face):
    return ref[n * face : (n + 1) * face, :]


def send_faces(values_ref, table_ref, outs, face):
    up_x, up_y, low_x, low_y = outs
    up_x[...] = wide_sum(dot(table_ref[0], wide_two(faces_of(values_ref, 1, face))))
    up_y[...] = wide_sum(dot(table_ref[1], wide_two(faces_of(values_ref, 3, face))))
    low_x[...] = faces_of(values_ref, 0, face)
    low_y[...] = faces_of(values_ref, 2, face)


def jump_faces(values_ref, received, table_ref, face):
    below_x, below_y, above_x, above_y = received
    up = [wide_sum(dot_columns(table_ref[a], wide_two(ref[...]))) for a, ref in ((0, above_x), (1, above_y))]
    own = [faces_of(values_ref, n, face) for n in range(6)]
    return [
        own[0] - below_x[...], own[1] - up[0], own[2] - below_y[...], own[3] - up[1], 0.0 * own[4], 0.0 * own[5]
    ]


def column_sum(a, b):
    return jnp.sum(a * b, axis=0, keepdims=True)


def write_rows(ref, rows):
    ref[...] = jnp.concatenate([*rows, jnp.zeros((8 - len(rows), rows[0].shape[1]), F32)], axis=0)


def loads_of(solved_ref, reach_ref, energy, ids, face):
    loads = jnp.zeros((128, 2 * 128), F32)
    for n in range(4):
        loads += dot(reach_ref[n], wide_two(faces_of(solved_ref, n, face)))
    loads = 0.5 * wide_sum(loads)
    row = lax.broadcasted_iota(jnp.int32, (128, 128), 0)
    loads = jnp.where(row == E_LANE, energy, loads)
    if ids is not None:
        number = jnp.where(row == ID_LANE, ids[0], jnp.where(row == ID_LANE + 1, ids[1], 0))
        loads = loads + number.astype(F32)
    return loads.T


def corner_faces(corners, reach_ref):
    pieces = wide_two(corners)
    return [wide_sum(dot_columns(reach_ref[n], pieces)) for n in range(4)]


def coupling_of(phi_ref, n, face):
    return phi_ref[...].astype(F32)[:, n * face : (n + 1) * face]


def start_kernel(rhs_ref, pairing_ref, phi_ref, plus_x, plus_y, minus_x, minus_y, table_ref):
    face = rhs_ref.shape[1]
    row = lax.broadcasted_iota(jnp.int32, (face, face), 0)
    for a, (plus, minus) in enumerate(((plus_x, minus_x), (plus_y, minus_y))):
        table = jnp.where(row == pairing_ref[a], 1.0, 0.0).astype(BF16)
        table_ref[a] = table
        plus[0:face, :] = wide_sum(dot(table, wide_two(rhs_ref[a])))
        moved = dot_rows(coupling_of(phi_ref, 2 * a + 1, face).astype(BF16), table)
        moved = jnp.concatenate([moved, jnp.zeros((24, 256 - face), F32)], axis=1)
        plus[face : face + 24, :] = moved[:, :128]
        plus[face + 24 : face + 48, :] = moved[:, 128:]
        minus[...] = coupling_of(phi_ref, 2 * a, face)


def rows_by_component(rows_ref, held_ref):
    source = lax.broadcasted_iota(jnp.int32, (128, 384), 0)
    target = lax.broadcasted_iota(jnp.int32, (128, 384), 1)
    wanted = 3 * (target % 128) + target // 128
    total = jnp.zeros((24, 384), F32)
    for m in range(3):
        chosen = jnp.where(wanted == 128 * m + source, 1.0, 0.0).astype(BF16)
        part = [rows_ref[:, (3 * q + m) * 128 : (3 * q + m + 1) * 128] for q in range(4)]
        part = jnp.concatenate(part, axis=0)
        high = part.astype(BF16)
        total += dot(high, chosen) + dot((part - high.astype(F32)).astype(BF16), chosen)
    for q in range(4):
        for column in range(3):
            for i in range(3):
                for b in range(2):
                    at = q * 18 + column * 6 + i * 2 + b
                    held_ref[at : at + 1, :] = total[q * 6 + b * 3 + i : q * 6 + b * 3 + i + 1, column * 128 : (column + 1) * 128]


def first_kernel(
    ids_ref, rhs_ref, below_x, below_y, above_x, above_y, phi_ref, table_ref, matrix_ref, rows_ref,
    half_ref, solved_ref, reach_ref, up_x, up_y, low_x, low_y, out_ref, held_ref,
):
    face = rhs_ref.shape[1]
    none = jnp.zeros((face, 128), F32)
    half = [
        -0.5 * below_x[0:face, :], 0.5 * rhs_ref[0], -0.5 * below_y[0:face, :], 0.5 * rhs_ref[1], none, 0.0 * rhs_ref[2]
    ]
    for n in range(6):
        half_ref[n * face : (n + 1) * face, :] = half[n]
    solved_ref[...] = dot(matrix_ref[...], half_ref[...].astype(BF16))
    send_faces(solved_ref, table_ref, (up_x, up_y, low_x, low_y), face)

    def near(n, slot, other):
        parts = [coupling_of(phi_ref, n, face)] + [jnp.zeros((24, face), F32)] * 4 + [jnp.zeros((8, face), F32)]
        parts[slot] = -other
        reach_ref[n] = jnp.concatenate(parts, axis=0).astype(BF16)

    for a, (below, above) in enumerate(((below_x, above_x), (below_y, above_y))):
        near(2 * a + 1, 1 + 2 * a, dot(above[...].astype(BF16), table_ref[a]))
        under = jnp.concatenate([below[face : face + 24, :], below[face + 24 : face + 48, :]], axis=1)
        near(2 * a, 2 + 2 * a, under[:, :face])
    energy = column_sum(half_ref[...], solved_ref[...])
    loads = loads_of(solved_ref, reach_ref, energy, (ids_ref[0], ids_ref[4]), face)
    rows_by_component(rows_ref, held_ref)
    for x in range(GX):
        out_ref[x, 0:CHUNK, :] = loads[x * CHUNK : (x + 1) * CHUNK]
        out_ref[x, CHUNK : CHUNK + 72, :] = held_ref[...]


def stretch_kernel(
    solved_ref, below_x, below_y, above_x, above_y, table_ref, matrix_ref, *rest
):
    face = below_x.shape[0]
    old = rest[:2] if len(rest) == 10 else None
    field_ref, stretched_ref, upper_ref, up_x, up_y, low_x, low_y, sums_ref = rest[-8:]
    jumped = jump_faces(solved_ref, (below_x, below_y, above_x, above_y), table_ref, face)
    for n in range(6):
        field_ref[n * face : (n + 1) * face, :] = 0.5 * jumped[n]
        if n % 2 == 1:
            upper_ref[n // 2] = 0.5 * jumped[n]
    stretched_ref[...] = dot(matrix_ref[...], field_ref[...].astype(BF16))
    send_faces(stretched_ref, table_ref, (up_x, up_y, low_x, low_y), face)
    rows = [column_sum(field_ref[...], stretched_ref[...])]
    if old is not None:
        old_field, old_stretched = old
        rows.append(
            column_sum(field_ref[...], old_stretched[...]) + column_sum(old_field[...], stretched_ref[...])
        )
    write_rows(sums_ref, rows)


def returned(got_ref):
    corners = jnp.concatenate([got_ref[x, 0:CHUNK, :] for x in range(GX)], axis=0).T
    sums = got_ref[0, CHUNK:, :]
    for x in range(1, GX):
        sums += got_ref[x, CHUNK:, :]
    return corners, sums


def turn_kernel(
    got_ref, half_ref, stretched_ref, below_x, below_y, above_x, above_y, table_ref, reach_ref, matrix_ref,
    next_ref, solved_ref, image_ref, corners_ref, scalars_ref, up_x, up_y, low_x, low_y, out_ref,
):
    face = below_x.shape[0]
    corners, sums = returned(got_ref)
    corners_ref[...] = corners
    energy = corners[E_LANE : E_LANE + 1]
    curvature = sums[0:1] + corners[E_LANE + 1 : E_LANE + 2]
    alpha = energy / curvature
    write_rows(scalars_ref, [energy, curvature, alpha])
    jumped = jump_faces(stretched_ref, (below_x, below_y, above_x, above_y), table_ref, face)
    coarse = corner_faces(corners, reach_ref)
    for n in range(6):
        at = slice(n * face, (n + 1) * face)
        image = jumped[n] + coarse[n] if n < 4 else jumped[n]
        image_ref[at, :] = image
        next_ref[at, :] = half_ref[at, :] - (0.5 * alpha) * image
    solved_ref[...] = dot(matrix_ref[...], next_ref[...].astype(BF16))
    send_faces(solved_ref, table_ref, (up_x, up_y, low_x, low_y), face)
    energy = column_sum(next_ref[...], solved_ref[...])
    loads = loads_of(solved_ref, reach_ref, energy, None, face)
    for x in range(GX):
        out_ref[x] = loads[x * CHUNK : (x + 1) * CHUNK]


def last_kernel(
    got_ref, half_ref, upper_ref, fresh_ref, stretched_ref, below_x, below_y, above_x, above_y, image_ref,
    corners_ref, scalars_ref, table_ref, reach_ref, matrix_ref, multipliers_ref, out_ref, held_ref,
):
    face = below_x.shape[0]
    corners, sums = returned(got_ref)
    start, curvature, alpha = scalars_ref[0:1], scalars_ref[1:2], scalars_ref[2:3]
    energy = corners[E_LANE : E_LANE + 1]
    ratio = energy / start
    mixed = sums[1:2] + 2.0 * corners[E_LANE + 2 : E_LANE + 3]
    curvature = sums[0:1] + corners[E_LANE + 1 : E_LANE + 2] + ratio * mixed + ratio * ratio * curvature
    step = energy / curvature
    jumped = jump_faces(stretched_ref, (below_x, below_y, above_x, above_y), table_ref, face)
    coarse = corner_faces(corners, reach_ref)
    for n in range(6):
        at = slice(n * face, (n + 1) * face)
        image = jumped[n] + coarse[n] if n < 4 else jumped[n]
        held_ref[at, :] = half_ref[at, :] - (0.5 * step) * (image + ratio * image_ref[at, :])
    for a in range(3):
        first = upper_ref[a]
        multipliers_ref[a] = alpha * first + step * (fresh_ref[a] + ratio * first)
    solved = dot(matrix_ref[...], held_ref[...].astype(BF16))
    out_ref[...] = column_sum(held_ref[...], solved)


def call(kernel, outs, smem=0, scratch=(), flops=2_000_000, limit=VMEM_LIMIT):
    vmem = pl.BlockSpec(memory_space=pltpu.VMEM)

    def run(*operands, after=()):
        many = len(operands)

        def body(*refs):
            kernel(*refs[:many], *refs[many + len(after) :])

        specs = [pl.BlockSpec(memory_space=pltpu.SMEM)] * smem + [vmem] * (many - smem)
        return pl.pallas_call(
            body,
            name=kernel.__name__,
            out_shape=[jax.ShapeDtypeStruct(s, d) for s, d in outs],
            in_specs=specs + [pl.BlockSpec(memory_space=pl.ANY)] * len(after),
            out_specs=[vmem] * len(outs),
            scratch_shapes=list(scratch),
            compiler_params=pltpu.CompilerParams(vmem_limit_bytes=limit),
            cost_estimate=pl.CostEstimate(flops=flops, bytes_accessed=1_000_000, transcendentals=0),
        )(*operands, *after)

    return run


SENT = [((GYN, 8, 128), F32), ((CHUNK, 3 * NODES), F32), ((CHUNK, 128), F32)]
spread = call(spread_kernel, [((GYN, CHUNK, 256), F32)])
first_solve = call(
    first_solve_kernel,
    SENT + [((144, NODES), BF16), ((144, NODES), BF16), ((NODES, NODES), BF16)],
    smem=1,
    scratch=[pltpu.VMEM((144, NODES), F32)],
)
next_solve = call(next_solve_kernel, SENT, smem=1)
pick = call(pick_kernel, [((GX, CHUNK + 8, 128), F32), ((3 * CHUNK, NODES), F32)])


def passed_along(array, axis, by):
    peers = lax.axis_size(axis)
    return lax.ppermute(array, axis, [(i, (i + by) % peers) for i in range(peers)])


def passed_both_ways(up_x, up_y, low_x, low_y):
    return (
        passed_along(up_x, "gx", 1),
        passed_along(up_y, GY, 1),
        passed_along(low_x, "gx", -1),
        passed_along(low_y, GY, -1),
    )


def exchanged(array, axis):
    return lax.all_to_all(array, axis, split_axis=0, concat_axis=0, tiled=True)


def local(rhs, stiff_inverse, schur, phi, coarse_inverse, incidence, pairing):
    face = rhs.shape[4]
    interface = 6 * face
    rhs = rhs[0, 0, 0]
    stiffness = stiff_inverse[0, 0, 0]
    schur_block = schur[0, 0, 0]
    pairing = pairing[0, 0, 0].reshape(3, 1, face)
    coupling = phi[0, 0, 0]
    me = lax.axis_index(GY).astype(jnp.int32).reshape(1)
    lanes = (jnp.asarray(corner_lanes())[:, None] == jnp.arange(256)[None, :]).astype(BF16)
    whole, upper, faces = ((interface, 128), F32), ((3, face, 128), F32), [((face, 128), F32)] * 4
    big = 2 * interface * interface * 128
    *sent, table = call(
        start_kernel, [((face + 48, 128), F32)] * 2 + [((24, face), F32)] * 2 + [((2, face, face), BF16)],
        limit=None,
    )(rhs, pairing, coupling)
    received = passed_both_ways(*sent)
    half, solved, reach, *sent, message = call(
        first_kernel,
        [whole, whole, ((4, 128, face), BF16), *faces, ((GX, CHUNK + 72, 128), F32)],
        smem=1,
        scratch=[pltpu.VMEM((72, 128), F32)],
        flops=big,
        limit=None,
    )(incidence[0, 0, 0], rhs, *received, coupling, table, schur_block, coarse_inverse)
    received = passed_both_ways(*sent)
    first_rows = exchanged(message, "gx")
    (sent,) = spread(first_rows, lanes, after=received)
    field, stretched, direction, *faces_sent, sums = call(stretch_kernel, [whole, whole, upper, *faces, ((8, 128), F32)], flops=big)(
        solved, *received, table, stiffness
    )
    received = passed_both_ways(*faces_sent)
    arrived = exchanged(sent, GY)
    sent, loads, energy, high, low, place = first_solve(me, arrived, first_rows, sums)
    back, grid = pick(exchanged(sent, GY), loads, energy, place, lanes, after=received)
    back = exchanged(back, "gx")
    half, solved, image, corners, scalars, *sent, message = call(
        turn_kernel,
        [whole, whole, whole, ((128, 128), F32), ((8, 128), F32), *faces, ((GX, CHUNK, 128), F32)],
        flops=big,
    )(back, half, stretched, *received, table, reach, schur_block)

    received = passed_both_ways(*sent)
    (sent,) = spread(exchanged(message, "gx"), lanes, after=received)
    _, fresh_stretched, fresh, *faces_sent, sums = call(
        stretch_kernel, [whole, whole, upper, *faces, ((8, 128), F32)], flops=big
    )(solved, *received, table, stiffness, field, stretched)
    received = passed_both_ways(*faces_sent)
    sent, loads, energy = next_solve(me, exchanged(sent, GY), high, low, sums)
    back, _ = pick(exchanged(sent, GY), loads, energy, place, lanes, grid, after=received)
    back = exchanged(back, "gx")
    multipliers, energy = call(
        last_kernel,
        [((3, face, 128), F32), ((1, 128), F32)],
        scratch=[pltpu.VMEM((interface, 128), F32)],
        flops=big,
    )(
        back, half, direction, fresh, fresh_stretched, *received, image, corners, scalars, table, reach, schur_block
    )
    energy = jnp.sum(exchanged(jnp.broadcast_to(energy, (GX * GYN, 1, 128)), GX_GY), axis=(0, 1))
    return (multipliers[None, None, None], energy / scalars[0])


def solution(mesh):
    finer = Mesh(mesh.devices.reshape(mesh.shape["gx"], 4, 4, 2), ("gx", "gy_0", "gy_1", "gy_2"))
    in_specs = (
        P("gx", GY, None, None, None, None),
        P("gx", GY, None, None, None),
        P("gx", GY, None, None, None),
        P("gx", GY, None, None, None),
        P(GX_GY, None),
        P("gx", GY, None, None),
        P("gx", GY, None, None, None),
    )
    out_specs = (P("gx", GY, None, None, None, None), P())
    return jax.shard_map(local, mesh=finer, in_specs=in_specs, out_specs=out_specs, check_vma=False)
```

```python
import functools

import jax
import jax.numpy as jnp
import numpy as np
from jax import lax
from jax.experimental import pallas as pl
from jax.experimental.pallas import tpu as pltpu
from jax.sharding import Mesh
from jax.sharding import PartitionSpec as P

GY = ("gy_0", "gy_1", "gy_2")
GX_GY = ("gx", "gy_0", "gy_1", "gy_2")
EXACT = lax.Precision.HIGHEST
GX, GYN = 8, 32
CHUNK = 16
NODES = 2 * GX * GYN
VMEM_LIMIT = 55_000_000
E_LANE, ID_LANE = 120, 121
F32, BF16 = jnp.float32, jnp.bfloat16


def corner_lanes():
    lanes = np.full(128, -1, np.int32)
    shifts = [(0, 0), (1, 0), (-1, 0), (0, 1), (0, -1)]
    for t, (dx, dy) in enumerate(shifts):
        for c in range(8):
            for i in range(3):
                j = 1 + dy + (c // 2) % 2
                lanes[t * 24 + 3 * c + i] = j * 64 + i * 16 + (dx + c % 2) % GX * 2 + c // 4
    lanes[E_LANE], lanes[ID_LANE], lanes[ID_LANE + 1] = 48, 112, 113
    return lanes


def halves_of(a, axis):
    high = a.astype(BF16)
    low = (a - high.astype(F32)).astype(BF16)
    return jnp.concatenate([high, low], axis=axis)


def in_two(a):
    return halves_of(a, 0)


def added_up(stacked):
    rows = stacked.shape[0] // 2
    return stacked[:rows] + stacked[rows:]


def dot(a, b):
    return lax.dot_general(a, b, (((1,), (0,)), ((), ())), preferred_element_type=F32)


def dot_rows(a, b):
    return lax.dot_general(a, b, (((1,), (1,)), ((), ())), preferred_element_type=F32)


def moved_lanes(a, start, to):
    by = (to - start) % 128
    return a if by == 0 else pltpu.roll(a, by, 1)


def lane_group(shape):
    return lax.broadcasted_iota(jnp.int32, shape, 1) // 16


def rolled_groups(a, by):
    by %= 16
    if by == 0:
        return a
    lane = lax.broadcasted_iota(jnp.int32, (a.shape[0], 128), 1) % 16
    tiles = [a[:, n : n + 128] for n in range(0, a.shape[1], 128)]
    return jnp.concatenate(
        [jnp.where(lane >= by, pltpu.roll(t, by, 1), pltpu.roll(t, 112 + by, 1)) for t in tiles], axis=1
    )


def spread_kernel(got_ref, lanes_ref, out_ref):
    loads = jnp.concatenate([got_ref[x, 0:CHUNK, :] for x in range(GX)], axis=0)
    placed = added_up(dot(in_two(loads), lanes_ref[...]))
    total = placed[0:CHUNK]
    for x in range(1, GX):
        total += rolled_groups(placed[x * CHUNK : (x + 1) * CHUNK], 2 * x)
    out_ref[...] = jnp.broadcast_to(total[None], out_ref.shape)


def assembled_loads(me, got_ref, loads_ref):
    group = lane_group((CHUNK, 128))
    tiles = [[None] * 4 for _ in range(3)]
    energy = jnp.zeros((CHUNK, 128), F32)

    def left(k):
        return got_ref[lax.rem(me + (k + 31) % GYN, GYN), :, 0:128]

    def right(k):
        return got_ref[lax.rem(me + (k + 31) % GYN, GYN), :, 128:256]

    for k in range(GYN):
        low = right(k - 1) + left(k + 1)
        high = left(k) + right(k - 2)
        load = low + pltpu.roll(high, 64, 1)
        energy += left(k)
        for i in range(3):
            piece = jnp.where(group == k % 8, moved_lanes(load, i * 16, (k % 8) * 16), 0.0)
            old = tiles[i][k // 8]
            tiles[i][k // 8] = piece if old is None else old + piece
    for i in range(3):
        for q in range(4):
            loads_ref[:, i * 512 + q * 128 : i * 512 + (q + 1) * 128] = tiles[i][q]
    energy = jnp.sum(jnp.where(group == 3, energy, 0.0), axis=1, keepdims=True)
    return jnp.broadcast_to(energy, (CHUNK, 128))


def own_rows(loads_ref, high_ref, low_ref):
    total = jnp.zeros((CHUNK, 48), F32)
    for i in range(3):
        a = loads_ref[:, i * 512 : (i + 1) * 512]
        high = a.astype(BF16)
        low = (a - high.astype(F32)).astype(BF16)
        both = dot_rows(jnp.concatenate([high, low], axis=0), high_ref[i * 48 : (i + 1) * 48, :])
        total += both[:CHUNK] + both[CHUNK:] + dot_rows(high, low_ref[i * 48 : (i + 1) * 48, :])
    return total


def send_rows(rows, energy, sums_ref, out_ref, energy_ref):
    wide = jnp.concatenate([rows, jnp.zeros((CHUNK, 80), F32)], axis=1)
    tile = wide[0:8] + pltpu.roll(wide[8:16], 48, 1)
    row = lax.broadcasted_iota(jnp.int32, (8, 128), 0)
    group = lane_group((8, 128))
    for n in range(2):
        spread_row = jnp.broadcast_to(sums_ref[n : n + 1, :], (8, 128))
        for r in range(8):
            here = (row == r) & (group == 6 + n)
            tile = jnp.where(here, moved_lanes(spread_row, r * 16, 96 + n * 16), tile)
    out_ref[...] = jnp.broadcast_to(tile[None], (GYN, 8, 128))
    energy_ref[...] = energy


def rows_of_sums(tile):
    row = lax.broadcasted_iota(jnp.int32, (8, 128), 0)
    group = lane_group((8, 128))
    out = jnp.zeros((8, 128), F32)
    for n in range(2):
        for r in range(8):
            whole = jnp.broadcast_to(tile[r : r + 1, :], (8, 128))
            out = jnp.where((row == n) & (group == r), moved_lanes(whole, 96 + n * 16, r * 16), out)
    return out


def first_solve_kernel(
    me_ref, got_ref, rows_ref, sums_ref, out_ref, loads_ref, energy_ref, high_ref, low_ref, place_ref, held
):
    me = me_ref[0]
    energy = assembled_loads(me, got_ref, loads_ref)
    group = lane_group((8, 128))
    ids = []
    for q in range(4):
        tile = jnp.zeros((8, 128), F32)
        for n in range(8):
            left = got_ref[lax.rem(me + (q * 8 + n + 31) % GYN, GYN), 0:8, 0:128]
            tile += jnp.where(group == n, moved_lanes(left, 112, n * 16), 0.0)
        ids.append(tile[0:1])
    ids = jnp.concatenate(ids, axis=1).astype(jnp.int32)
    row = lax.broadcasted_iota(jnp.int32, (NODES, NODES), 0)
    by_id = jnp.where(row == ids, 1.0, 0.0).astype(BF16)
    place = (ids % 64 // 2) * 16 + (ids // 64) * 2 + ids % 2
    place_ref[...] = jnp.where(row == place, 1.0, 0.0).astype(BF16)
    for x in range(GX):
        for q in range(4):
            for column in range(3):
                for i in range(3):
                    start = CHUNK + q * 18 + column * 6 + i * 2
                    at = column * 48 + i * 16 + x * 2
                    held[at : at + 2, q * 128 : (q + 1) * 128] = rows_ref[x, start : start + 2, :]
    ordered = added_up(dot(in_two(held[...]), by_id))
    high = ordered.astype(BF16)
    high_ref[...] = high
    low_ref[...] = (ordered - high.astype(F32)).astype(BF16)
    rows = own_rows(loads_ref, high_ref, low_ref)
    send_rows(rows, energy, sums_ref, out_ref, energy_ref)


def next_solve_kernel(me_ref, got_ref, high_ref, low_ref, sums_ref, out_ref, loads_ref, energy_ref):
    energy = assembled_loads(me_ref[0], got_ref, loads_ref)
    rows = own_rows(loads_ref, high_ref, low_ref)
    send_rows(rows, energy, sums_ref, out_ref, energy_ref)


def lane_sum(a, b_ref, shape):
    total = jnp.zeros((CHUNK, 1), F32)
    for i in range(3):
        total += jnp.sum(a[:, i * 512 : (i + 1) * 512] * b_ref[i * CHUNK : (i + 1) * CHUNK, :], axis=1, keepdims=True)
    return jnp.broadcast_to(total, shape)


def pick_kernel(got_ref, loads_ref, energy_ref, place_ref, lanes_ref, *rest):
    before_ref = rest[0] if len(rest) == 3 else None
    out_ref, grid_ref = rest[-2:]
    group = lane_group((CHUNK, 128))
    tiles = [[None] * 4 for _ in range(3)]
    sums = jnp.zeros((8, 128), F32)
    for k in range(GYN):
        rows = got_ref[k]
        sums += rows
        for i in range(3):
            to = (k % 8) * 16
            both = [moved_lanes(rows, i * 16, to), moved_lanes(rows, 48 + i * 16, to)]
            piece = jnp.where(group == k % 8, jnp.concatenate(both, axis=0), 0.0)
            old = tiles[i][k // 8]
            tiles[i][k // 8] = piece if old is None else old + piece
    solution = jnp.concatenate([jnp.concatenate(tiles[i], axis=1) for i in range(3)], axis=0)
    grid_ref[...] = added_up(dot(in_two(solution), place_ref[...]))
    loads = loads_ref[...]
    shape = (CHUNK, 128)
    product = lane_sum(loads, grid_ref, shape)
    mixed = product if before_ref is None else lane_sum(loads, before_ref, shape)
    lane = lax.broadcasted_iota(jnp.int32, shape, 1)
    halves = []
    for half in range(2):
        tile = jnp.zeros(shape, F32)
        for n in range(2):
            for i in range(3):
                at = n * 64 + i * 16
                near = grid_ref[i * CHUNK : (i + 1) * CHUNK, 0:128]
                tile = jnp.where(group == at // 16, moved_lanes(near, (half * 2 + n) * 16, at), tile)
        if half == 0:
            tile = jnp.where(group == 3, energy_ref[...], tile)
            tile = jnp.where(lane >= 112, jnp.where(lane % 2 == 0, product, mixed), tile)
        halves.append(tile)
    near = jnp.concatenate(halves, axis=1)
    near = jnp.concatenate([rolled_groups(near, -2 * x) for x in range(GX)], axis=0)
    picked = added_up(dot_rows(in_two(near), lanes_ref[...]))
    sums = rows_of_sums(sums)
    for x in range(GX):
        out_ref[x, 0:CHUNK, :] = picked[x * CHUNK : (x + 1) * CHUNK]
        out_ref[x, CHUNK : CHUNK + 8, :] = sums


def wide_two(a):
    return halves_of(a, 1)


def wide_sum(a):
    width = a.shape[1] // 2
    return a[:, :width] + a[:, width:]


def dot_columns(a, b):
    return lax.dot_general(a, b, (((0,), (0,)), ((), ())), preferred_element_type=F32)


def faces_of(ref, n, face):
    return ref[n * face : (n + 1) * face, :]


def send_faces(values_ref, table_ref, outs, face):
    up_x, up_y, low_x, low_y = outs
    up_x[...] = wide_sum(dot(table_ref[0], wide_two(faces_of(values_ref, 1, face))))
    up_y[...] = wide_sum(dot(table_ref[1], wide_two(faces_of(values_ref, 3, face))))
    low_x[...] = faces_of(values_ref, 0, face)
    low_y[...] = faces_of(values_ref, 2, face)


def jump_faces(values_ref, received, table_ref, face, multiply=dot_columns):
    below_x, below_y, above_x, above_y = received
    up = [wide_sum(multiply(table_ref[a], wide_two(ref[...]))) for a, ref in ((0, above_x), (1, above_y))]
    own = [faces_of(values_ref, n, face) for n in range(6)]
    return [
        own[0] - below_x[...], own[1] - up[0], own[2] - below_y[...], own[3] - up[1], 0.0 * own[4], 0.0 * own[5]
    ]


def column_sum(a, b):
    return jnp.sum(a * b, axis=0, keepdims=True)


def write_rows(ref, rows):
    ref[...] = jnp.concatenate([*rows, jnp.zeros((8 - len(rows), rows[0].shape[1]), F32)], axis=0)


def loads_of(solved_ref, reach_ref, energy, ids, face):
    loads = jnp.zeros((128, 2 * 128), F32)
    for n in range(4):
        loads += dot(reach_ref[n], wide_two(faces_of(solved_ref, n, face)))
    loads = 0.5 * wide_sum(loads)
    row = lax.broadcasted_iota(jnp.int32, (128, 128), 0)
    loads = jnp.where(row == E_LANE, energy, loads)
    if ids is not None:
        number = jnp.where(row == ID_LANE, ids[0], jnp.where(row == ID_LANE + 1, ids[1], 0))
        loads = loads + number.astype(F32)
    return loads.T


def corner_faces(corners, reach_ref):
    pieces = wide_two(corners)
    return [wide_sum(dot(reach_ref[n], pieces)) for n in range(4)]


def coupling_of(phi_ref, n, face):
    return phi_ref[...].astype(F32)[:, n * face : (n + 1) * face]


def start_kernel(rhs_ref, pairing_ref, phi_ref, plus_x, plus_y, minus_x, minus_y, table_ref):
    face = rhs_ref.shape[1]
    row = lax.broadcasted_iota(jnp.int32, (face, face), 0)
    for a, (plus, minus) in enumerate(((plus_x, minus_x), (plus_y, minus_y))):
        table = jnp.where(row == pairing_ref[a], 1.0, 0.0).astype(BF16)
        table_ref[a] = table
        plus[0:face, :] = wide_sum(dot(table, wide_two(rhs_ref[a])))
        moved = dot_rows(coupling_of(phi_ref, 2 * a + 1, face).astype(BF16), table)
        moved = jnp.concatenate([moved, jnp.zeros((24, 256 - face), F32)], axis=1)
        plus[face : face + 24, :] = moved[:, :128]
        plus[face + 24 : face + 48, :] = moved[:, 128:]
        minus[...] = coupling_of(phi_ref, 2 * a, face)


def rows_by_component(rows_ref, held_ref):
    source = lax.broadcasted_iota(jnp.int32, (128, 384), 0)
    target = lax.broadcasted_iota(jnp.int32, (128, 384), 1)
    wanted = 3 * (target % 128) + target // 128
    total = jnp.zeros((24, 384), F32)
    for m in range(3):
        chosen = jnp.where(wanted == 128 * m + source, 1.0, 0.0).astype(BF16)
        part = [rows_ref[:, (3 * q + m) * 128 : (3 * q + m + 1) * 128] for q in range(4)]
        part = jnp.concatenate(part, axis=0)
        high = part.astype(BF16)
        total += dot(high, chosen) + dot((part - high.astype(F32)).astype(BF16), chosen)
    for q in range(4):
        for column in range(3):
            for i in range(3):
                for b in range(2):
                    at = q * 18 + column * 6 + i * 2 + b
                    held_ref[at : at + 1, :] = total[q * 6 + b * 3 + i : q * 6 + b * 3 + i + 1, column * 128 : (column + 1) * 128]


def first_kernel(
    ids_ref, rhs_ref, below_x, below_y, above_x, above_y, phi_ref, table_ref, matrix_ref, rows_ref,
    half_ref, solved_ref, reach_ref, up_x, up_y, low_x, low_y, out_ref, held_ref,
):
    face = rhs_ref.shape[1]
    none = jnp.zeros((face, 128), F32)
    half = [
        -0.5 * below_x[0:face, :], 0.5 * rhs_ref[0], -0.5 * below_y[0:face, :], 0.5 * rhs_ref[1], none, 0.0 * rhs_ref[2]
    ]
    for n in range(6):
        half_ref[n * face : (n + 1) * face, :] = half[n]
    solved_ref[...] = dot(matrix_ref[...], half_ref[...].astype(BF16))
    send_faces(solved_ref, table_ref, (up_x, up_y, low_x, low_y), face)

    def near(n, slot, other):
        parts = [coupling_of(phi_ref, n, face)] + [jnp.zeros((24, face), F32)] * 4 + [jnp.zeros((8, face), F32)]
        parts[slot] = -other
        reach_ref[n] = jnp.concatenate(parts, axis=0).astype(BF16)

    for a, (below, above) in enumerate(((below_x, above_x), (below_y, above_y))):
        near(2 * a + 1, 1 + 2 * a, dot(above[...].astype(BF16), table_ref[a]))
        under = jnp.concatenate([below[face : face + 24, :], below[face + 24 : face + 48, :]], axis=1)
        near(2 * a, 2 + 2 * a, under[:, :face])
    energy = column_sum(half_ref[...], solved_ref[...])
    loads = loads_of(solved_ref, reach_ref, energy, (ids_ref[0], ids_ref[4]), face)
    rows_by_component(rows_ref, held_ref)
    for x in range(GX):
        out_ref[x, 0:CHUNK, :] = loads[x * CHUNK : (x + 1) * CHUNK]
        out_ref[x, CHUNK : CHUNK + 72, :] = held_ref[...]


def stretch_kernel(
    solved_ref, below_x, below_y, above_x, above_y, table_ref, matrix_ref, *rest
):
    face = below_x.shape[0]
    old = rest[:2] if len(rest) == 10 else None
    field_ref, stretched_ref, upper_ref, up_x, up_y, low_x, low_y, sums_ref = rest[-8:]
    jumped = jump_faces(solved_ref, (below_x, below_y, above_x, above_y), table_ref, face)
    for n in range(6):
        field_ref[n * face : (n + 1) * face, :] = 0.5 * jumped[n]
        if n % 2 == 1:
            upper_ref[n // 2] = 0.5 * jumped[n]
    stretched_ref[...] = dot(matrix_ref[...], field_ref[...].astype(BF16))
    send_faces(stretched_ref, table_ref, (up_x, up_y, low_x, low_y), face)
    rows = [column_sum(field_ref[...], stretched_ref[...])]
    if old is not None:
        old_field, old_stretched = old
        rows.append(
            column_sum(field_ref[...], old_stretched[...]) + column_sum(old_field[...], stretched_ref[...])
        )
    write_rows(sums_ref, rows)


def first_stretch_kernel(
    solved_ref, below_x, below_y, above_x, above_y, table_ref, matrix_ref, reach_ref, *outs
):
    turned_ref, spread_ref = outs[-2:]
    face = below_x.shape[0]
    row = lax.broadcasted_iota(jnp.int32, (face, face), 0)
    same = jnp.where(row == lax.broadcasted_iota(jnp.int32, (face, face), 1), 1.0, 0.0).astype(BF16)
    stretch_kernel(solved_ref, below_x, below_y, above_x, above_y, table_ref, matrix_ref, *outs[:-2])
    for a in range(2):
        turned_ref[a] = dot_columns(table_ref[a], same).astype(BF16)
    for n in range(4):
        spread_ref[n] = dot_rows(same, reach_ref[n]).astype(BF16)


def returned(got_ref):
    corners = jnp.concatenate([got_ref[x, 0:CHUNK, :] for x in range(GX)], axis=0).T
    sums = got_ref[0, CHUNK:, :]
    for x in range(1, GX):
        sums += got_ref[x, CHUNK:, :]
    return corners, sums


def turn_kernel(
    got_ref, half_ref, stretched_ref, below_x, below_y, above_x, above_y, table_ref, reach_ref, matrix_ref,
    turned_ref, across_ref, next_ref, solved_ref, image_ref, corners_ref, scalars_ref, up_x, up_y, low_x, low_y, out_ref,
):
    face = below_x.shape[0]
    corners, sums = returned(got_ref)
    corners_ref[...] = corners
    energy = corners[E_LANE : E_LANE + 1]
    curvature = sums[0:1] + corners[E_LANE + 1 : E_LANE + 2]
    alpha = energy / curvature
    write_rows(scalars_ref, [energy, curvature, alpha])
    jumped = jump_faces(stretched_ref, (below_x, below_y, above_x, above_y), turned_ref, face, dot)
    coarse = corner_faces(corners, across_ref)
    for n in range(6):
        at = slice(n * face, (n + 1) * face)
        image = jumped[n] + coarse[n] if n < 4 else jumped[n]
        image_ref[at, :] = image
        next_ref[at, :] = half_ref[at, :] - (0.5 * alpha) * image
    solved_ref[...] = dot(matrix_ref[...], next_ref[...].astype(BF16))
    send_faces(solved_ref, table_ref, (up_x, up_y, low_x, low_y), face)
    energy = column_sum(next_ref[...], solved_ref[...])
    loads = loads_of(solved_ref, reach_ref, energy, None, face)
    for x in range(GX):
        out_ref[x] = loads[x * CHUNK : (x + 1) * CHUNK]


def last_kernel(
    got_ref, half_ref, upper_ref, fresh_ref, stretched_ref, below_x, below_y, above_x, above_y, image_ref,
    corners_ref, scalars_ref, turned_ref, across_ref, matrix_ref, multipliers_ref, out_ref, held_ref,
):
    face = below_x.shape[0]
    corners, sums = returned(got_ref)
    start, curvature, alpha = scalars_ref[0:1], scalars_ref[1:2], scalars_ref[2:3]
    energy = corners[E_LANE : E_LANE + 1]
    ratio = energy / start
    mixed = sums[1:2] + 2.0 * corners[E_LANE + 2 : E_LANE + 3]
    curvature = sums[0:1] + corners[E_LANE + 1 : E_LANE + 2] + ratio * mixed + ratio * ratio * curvature
    step = energy / curvature
    jumped = jump_faces(stretched_ref, (below_x, below_y, above_x, above_y), turned_ref, face, dot)
    coarse = corner_faces(corners, across_ref)
    for n in range(6):
        at = slice(n * face, (n + 1) * face)
        image = jumped[n] + coarse[n] if n < 4 else jumped[n]
        held_ref[at, :] = half_ref[at, :] - (0.5 * step) * (image + ratio * image_ref[at, :])
    for a in range(3):
        first = upper_ref[a]
        multipliers_ref[a] = alpha * first + step * (fresh_ref[a] + ratio * first)
    solved = dot(matrix_ref[...], held_ref[...].astype(BF16))
    out_ref[...] = column_sum(held_ref[...], solved)


def call(kernel, outs, smem=0, scratch=(), flops=2_000_000, limit=VMEM_LIMIT):
    vmem = pl.BlockSpec(memory_space=pltpu.VMEM)

    def run(*operands, after=()):
        many = len(operands)

        def body(*refs):
            kernel(*refs[:many], *refs[many + len(after) :])

        specs = [pl.BlockSpec(memory_space=pltpu.SMEM)] * smem + [vmem] * (many - smem)
        return pl.pallas_call(
            body,
            name=kernel.__name__,
            out_shape=[jax.ShapeDtypeStruct(s, d) for s, d in outs],
            in_specs=specs + [pl.BlockSpec(memory_space=pl.ANY)] * len(after),
            out_specs=[vmem] * len(outs),
            scratch_shapes=list(scratch),
            compiler_params=pltpu.CompilerParams(vmem_limit_bytes=limit),
            cost_estimate=pl.CostEstimate(flops=flops, bytes_accessed=1_000_000, transcendentals=0),
        )(*operands, *after)

    return run


SENT = [((GYN, 8, 128), F32), ((CHUNK, 3 * NODES), F32), ((CHUNK, 128), F32)]
spread = call(spread_kernel, [((GYN, CHUNK, 256), F32)])
first_solve = call(
    first_solve_kernel,
    SENT + [((144, NODES), BF16), ((144, NODES), BF16), ((NODES, NODES), BF16)],
    smem=1,
    scratch=[pltpu.VMEM((144, NODES), F32)],
)
next_solve = call(next_solve_kernel, SENT, smem=1)
pick = call(pick_kernel, [((GX, CHUNK + 8, 128), F32), ((3 * CHUNK, NODES), F32)])


def passed_along(array, axis, by):
    peers = lax.axis_size(axis)
    return lax.ppermute(array, axis, [(i, (i + by) % peers) for i in range(peers)])


def passed_both_ways(up_x, up_y, low_x, low_y):
    return (
        passed_along(up_x, "gx", 1),
        passed_along(up_y, GY, 1),
        passed_along(low_x, "gx", -1),
        passed_along(low_y, GY, -1),
    )


def exchanged(array, axis):
    return lax.all_to_all(array, axis, split_axis=0, concat_axis=0, tiled=True)


def local(rhs, stiff_inverse, schur, phi, coarse_inverse, incidence, pairing):
    face = rhs.shape[4]
    interface = 6 * face
    rhs = rhs[0, 0, 0]
    stiffness = stiff_inverse[0, 0, 0]
    schur_block = schur[0, 0, 0]
    pairing = pairing[0, 0, 0].reshape(3, 1, face)
    coupling = phi[0, 0, 0]
    me = lax.axis_index(GY).astype(jnp.int32).reshape(1)
    lanes = (jnp.asarray(corner_lanes())[:, None] == jnp.arange(256)[None, :]).astype(BF16)
    whole, upper, faces = ((interface, 128), F32), ((3, face, 128), F32), [((face, 128), F32)] * 4
    big = 2 * interface * interface * 128
    *sent, table = call(
        start_kernel, [((face + 48, 128), F32)] * 2 + [((24, face), F32)] * 2 + [((2, face, face), BF16)],
        limit=None,
    )(rhs, pairing, coupling)
    received = passed_both_ways(*sent)
    half, solved, reach, *sent, message = call(
        first_kernel,
        [whole, whole, ((4, 128, face), BF16), *faces, ((GX, CHUNK + 72, 128), F32)],
        smem=1,
        scratch=[pltpu.VMEM((72, 128), F32)],
        flops=big,
        limit=None,
    )(incidence[0, 0, 0], rhs, *received, coupling, table, schur_block, coarse_inverse)
    received = passed_both_ways(*sent)
    first_rows = exchanged(message, "gx")
    (sent,) = spread(first_rows, lanes, after=received)
    field, stretched, direction, *faces_sent, sums, turned, across = call(
        first_stretch_kernel,
        [whole, whole, upper, *faces, ((8, 128), F32), ((2, face, face), BF16), ((4, face, 128), BF16)],
        flops=big,
    )(solved, *received, table, stiffness, reach)
    received = passed_both_ways(*faces_sent)
    arrived = exchanged(sent, GY)
    sent, loads, energy, high, low, place = first_solve(me, arrived, first_rows, sums)
    back, grid = pick(exchanged(sent, GY), loads, energy, place, lanes, after=received)
    back = exchanged(back, "gx")
    half, solved, image, corners, scalars, *sent, message = call(
        turn_kernel,
        [whole, whole, whole, ((128, 128), F32), ((8, 128), F32), *faces, ((GX, CHUNK, 128), F32)],
        flops=big,
    )(back, half, stretched, *received, table, reach, schur_block, turned, across)

    received = passed_both_ways(*sent)
    (sent,) = spread(exchanged(message, "gx"), lanes, after=received)
    _, fresh_stretched, fresh, *faces_sent, sums = call(
        stretch_kernel, [whole, whole, upper, *faces, ((8, 128), F32)], flops=big
    )(solved, *received, table, stiffness, field, stretched)
    received = passed_both_ways(*faces_sent)
    sent, loads, energy = next_solve(me, exchanged(sent, GY), high, low, sums)
    back, _ = pick(exchanged(sent, GY), loads, energy, place, lanes, grid, after=received)
    back = exchanged(back, "gx")
    multipliers, energy = call(
        last_kernel,
        [((3, face, 128), F32), ((1, 128), F32)],
        scratch=[pltpu.VMEM((interface, 128), F32)],
        flops=big,
    )(
        back, half, direction, fresh, fresh_stretched, *received, image, corners, scalars, turned, across, schur_block
    )
    energy = jnp.sum(exchanged(jnp.broadcast_to(energy, (GX * GYN, 1, 128)), GX_GY), axis=(0, 1))
    return (multipliers[None, None, None], energy / scalars[0])


def solution(mesh):
    finer = Mesh(mesh.devices.reshape(mesh.shape["gx"], 4, 4, 2), ("gx", "gy_0", "gy_1", "gy_2"))
    in_specs = (
        P("gx", GY, None, None, None, None),
        P("gx", GY, None, None, None),
        P("gx", GY, None, None, None),
        P("gx", GY, None, None, None),
        P(GX_GY, None),
        P("gx", GY, None, None),
        P("gx", GY, None, None, None),
    )
    out_specs = (P("gx", GY, None, None, None, None), P())
    return jax.shard_map(local, mesh=finer, in_specs=in_specs, out_specs=out_specs, check_vma=False)
```
